512 devices in a mesh: gy: 128 (over y, z_lo, x), gz: 4 (over z_hi, core).
Axes of the slice: x: 4, y: 4, z: 16 (z_hi: 2, z_lo: 8; z = z_hi * 8 + z_lo), core: 2. Of those that a mesh axis runs over, the one named last changes fastest.
Arguments:
- fuel: float32 [2048, 16, 2048], P('gy', 'gz'), may hold values from -6 to 6
- oxidant: float32 [2048, 16, 2048], P('gy', 'gz'), may hold values from -6 to 6
- rate: float32 [2048, 16, 2048], P('gy', 'gz'), may hold values from 0.05 to 0.5
- velocity: float32 [3], replicated, may hold values from -0.3 to 0.3
- sketch_x: float32 [128, 2048], replicated, may hold values from -0.125 to 0.125
- sketch_y: float32 [128, 2048], replicated, may hold values from -0.125 to 0.125
Outputs:
- sketch: float32 [128, 2, 16, 128], P('gy', None, 'gz')
The draws below stay inside these ranges and needn't reach their ends.
All inputs are finite; a program needn't handle non-finite values.
Results may differ from the reference program's by a relative error of at most 0.00014.
Values sent between devices are 32-bit elements; how exact they have to be, the bound alone decides.
A program may use at most 64 MiB of HBM per device.

```python
import math
import jax
import jax.numpy as jnp
from jax import lax

X = 2048
K = 128
STEPS = 2
NY = 2048
NZ = 16


def block_levels(rng, extent, pieces, least, high):
    loudness, own = 1.0, jax.random.fold_in(rng, 6)
    for dim, parts in pieces:
        steps = jnp.exp(jax.random.uniform(jax.random.fold_in(own, dim), (parts,), jnp.float32, least / len(pieces), high / len(pieces)))
        loudness = loudness * jnp.repeat(steps, extent[dim] // parts).reshape([-1 if axis == dim else 1 for axis in range(len(extent))])
    return loudness


def bell_draw(rng, dims, spread, reach, split=(), kind=jnp.bfloat16):
    loudness = block_levels(rng, dims, split, -0.22, 0.18) if split else 1.0
    array = jax.random.normal(rng, dims, jnp.float32) * spread * loudness
    return jnp.minimum(jnp.maximum(array, -reach), reach).astype(kind)


def setup_inputs(seed: int = 0) -> dict:
    splits = jax.random.split(jax.random.key(seed), 7)
    fuel = bell_draw(splits[0], (NY, NZ, X), 1.0, 6.0, ((0, 128), (1, 4)), jnp.float32)
    oxidant = bell_draw(splits[1], (NY, NZ, X), 1.0, 6.0, ((0, 128), (1, 4)), jnp.float32)
    rate = jnp.clip(jnp.exp(math.log(0.5) - 2.3025851 * jax.random.uniform(splits[2], (NY, NZ, X), jnp.float32) ** block_levels(splits[2], (NY, NZ, X), ((0, 128), (1, 4)), -0.2, 0.2)), 0.05, 0.5)
    velocity = jnp.clip(jax.random.uniform(splits[3], (3,), jnp.float32, -0.3, 0.3), -0.3, 0.3)
    sketch_x = bell_draw(splits[4], (K, X), X ** -0.5, 0.125, (), jnp.float32)
    sketch_y = bell_draw(splits[5], (K, NY), NY ** -0.5, 0.125, (), jnp.float32)
    return {"fuel": fuel, "oxidant": oxidant, "rate": rate, "velocity": velocity, "sketch_x": sketch_x, "sketch_y": sketch_y}


def advance(padded, rate, velocity):
    core = padded[:, 1:-1, 1:-1, :]
    xpad = jnp.pad(core, ((0, 0), (0, 0), (0, 0), (1, 1)))
    east = xpad[..., 2:]
    west = xpad[..., :-2]
    north = padded[:, 2:, 1:-1, :]
    south = padded[:, :-2, 1:-1, :]
    upper = padded[:, 1:-1, 2:, :]
    lower = padded[:, 1:-1, :-2, :]
    lap = east + west + north + south + upper + lower - 6.0 * core
    adv = 0.5 * (velocity[0] * (east - west) + velocity[1] * (north - south) + velocity[2] * (upper - lower))
    react = rate * core[0] * core[1]
    new_fuel = core[0] + 0.1 * lap[0] - adv[0] - react
    new_oxid = core[1] + 0.05 * lap[1] - adv[1] + react
    return jnp.stack([new_fuel, new_oxid])


def reference(fuel, oxidant, rate, velocity, sketch_x, sketch_y):
    fields = jnp.stack([fuel, oxidant])
    for step in range(STEPS):
        padded = jnp.pad(fields, ((0, 0), (1, 1), (1, 1), (0, 0)))
        fields = advance(padded, rate, velocity)
    projected = jnp.einsum("kx,fyzx->kfyz", sketch_x, fields, precision=lax.Precision.HIGHEST)
    return jnp.einsum("kfyz,jy->kfzj", projected, sketch_y, precision=lax.Precision.HIGHEST)
```

```python
import functools

import jax
import jax.numpy as jnp
from jax import lax
from jax.experimental import pallas as pl
from jax.experimental.pallas import tpu as pltpu
from jax.sharding import PartitionSpec as P

F32, BF16 = jnp.float32, jnp.bfloat16
MESH = pl.DeviceIdType.MESH
NX, NZL, NY = 4, 8, 4
DEVS = NX * NZL * NY
NT = 16
ROWS = 16


def roll(v, shift, axis):
    shift %= v.shape[axis]
    return pltpu.roll(v, shift, axis) if shift else v


def split(v):
    high = v.astype(BF16)
    return high, (v - high.astype(F32)).astype(BF16)


def dot(a, b, dims):
    return lax.dot_general(a, b, (dims, ((), ())), preferred_element_type=F32)


def kernel(
    fuel, fuel4, oxid, oxid4, rate, vel, sx, sy, out,
    F, RR, HB, VB, UF, RC, CC, CG, LT, SX, SXH, SXL, SY, SYT, SYH, SYL,
    P1, ZD, PC, ZC, EA, ER, TA, TR, AE,
    s_vb, s_f, s_rr, s_sx, s_sy, far_s, far_r, ys, yr, ds, dr, zd_s, zd_r, zc_s, zc_r, ea_s, ea_r, ta_s, ta_r,
    x1, x2, y1, y2, zu, zd, go,
):
    gy, gz = lax.axis_index("gy"), lax.axis_index("gz")
    x, zl, y = gy % NX, (gy // NX) % NZL, gy // (NX * NZL)
    core = gz % 2
    inner = (gz == 1) | (gz == 2)
    rim = jnp.logical_not(inner)
    partner = {"gy": gy, "gz": gz + 1 - 2 * core}
    opposite = {"gy": gy, "gz": 3 - gz}

    def at(yy, zz, xx):
        return {"gy": (yy * NZL + zz) * NX + xx, "gz": gz}

    def signal(sem, device):
        pl.semaphore_signal(sem, inc=1, device_id=device, device_id_type=MESH)

    def remote(src, dst, send, recv, device):
        return pltpu.make_async_remote_copy(
            src_ref=src, dst_ref=dst, send_sem=send, recv_sem=recv, device_id=device, device_id_type=MESH
        )

    def plane(p):
        return p + core * (3 - 2 * p)

    for f, src in enumerate((fuel4, oxid4)):
        for j in range(4):
            pltpu.make_async_copy(src.at[:, j, :, plane(0), :], VB.at[:, :, f * 4 + j, :], s_vb).start()
    for f, src in enumerate((fuel, oxid)):
        for p in (3, 0, 1, 2):
            pltpu.make_async_copy(src.at[:, :, plane(p), :], F.at[pl.ds(1, ROWS), :, f * 4 + p, :], s_f).start()
    for p in range(4):
        for f in range(2):
            pltpu.make_async_copy(rate.at[:, :, plane(p), :], RR.at[:, :, f * 4 + p, :], s_rr).start()
    pltpu.make_async_copy(sx, SX, s_sx).start()
    pltpu.make_async_copy(sy, SY, s_sy).start()

    barrier = pltpu.get_barrier_semaphore()
    signal(barrier, partner)
    right, left = at(y, zl, (x + 1) % NX), at(y, zl, (x + NX - 1) % NX)
    front, back = at((y + 1) % NY, zl, x), at((y + NY - 1) % NY, zl, x)
    above, below = at(y, zl + 1, x), at(y, zl - 1, x)

    @pl.when(inner)
    def _():
        signal(barrier, opposite)

    @pl.when(rim)
    def _():
        for device in (right, left, front, back):
            signal(barrier, device)

        @pl.when(zl < NZL - 1)
        def _():
            signal(barrier, above)

        @pl.when(zl > 0)
        def _():
            signal(barrier, below)

        UF[...] = jnp.zeros_like(UF)
        ZC[...] = jnp.zeros_like(ZC)

    @pl.when(gy == 0)
    def _():
        F[0] = jnp.zeros((NT, 8, 128), F32)

    @pl.when(gy == DEVS - 1)
    def _():
        F[ROWS + 1] = jnp.zeros((NT, 8, 128), F32)

    @pl.when(inner)
    def _():
        pl.semaphore_wait(barrier, 2)

    @pl.when(rim & ((zl == 0) | (zl == NZL - 1)))
    def _():
        pl.semaphore_wait(barrier, 6)

    @pl.when(rim & (zl > 0) & (zl < NZL - 1))
    def _():
        pl.semaphore_wait(barrier, 7)

    def far(g):
        return remote(VB.at[g], UF.at[g], far_s.at[g], far_r.at[g], opposite)

    pltpu.make_async_copy(VB, VB, s_vb).wait()

    @pl.when(inner)
    def _():
        for g in range(4):
            far(g).start()

    def deck(f):
        return remote(
            F.at[pl.ds(1, ROWS), :, f * 4 + 3, :], HB.at[:, :, f * 4 + 3, :], ds.at[f], dr.at[f], partner
        )

    pltpu.make_async_copy(F.at[pl.ds(1, ROWS)], F.at[pl.ds(1, ROWS)], s_f).wait()
    for f in range(2):
        deck(f).start()

    @pl.when(rim)
    def _():
        signal(x1, right)
        signal(x1, left)
        pl.semaphore_wait(x1, 2)
        signal(x2, right)
        pl.semaphore_wait(x2, 1)
        signal(y1, front)
        signal(y1, back)
        pl.semaphore_wait(y1, 2)
        signal(y2, front)
        pl.semaphore_wait(y2, 1)

        @pl.when(zl == 0)
        def _():
            signal(zu, above)

        @pl.when(zl == NZL - 1)
        def _():
            signal(zd, below)

        @pl.when((zl > 0) & (zl < NZL // 2))
        def _():
            pl.semaphore_wait(zu, 1)
            signal(zu, above)
            pl.semaphore_wait(zd, 1)
            signal(zd, below)

        @pl.when((zl < NZL - 1) & (zl >= NZL // 2))
        def _():
            pl.semaphore_wait(zd, 1)
            signal(zd, below)
            pl.semaphore_wait(zu, 1)
            signal(zu, above)

        @pl.when(zl == 0)
        def _():
            pl.semaphore_wait(zd, 1)

        @pl.when(zl == NZL - 1)
        def _():
            pl.semaphore_wait(zu, 1)

        signal(go, partner)

    sub = lax.broadcasted_iota(jnp.int32, (8, 128), 0)
    lane = lax.broadcasted_iota(jnp.int32, (8, 128), 1)
    sp = sub % 4
    v0, v1 = 0.5 * vel[0], 0.5 * vel[1]
    v2 = 0.5 * vel[2] * (1 - 2 * core).astype(F32)
    alpha = jnp.where(sub < 4, 0.1, 0.05).astype(F32)
    zero = jnp.zeros((8, 128), F32)
    k0, kE, kW, kN, kS = 1.0 - 6.0 * alpha, alpha - v0, alpha + v0, alpha - v1, alpha + v1
    kP, kM = alpha - v2, alpha + v2
    sg = jnp.where(sub < 4, -1.0, 1.0).astype(F32)
    kMz = jnp.where(sp == 0, zero, kM)
    kPz = jnp.where(sp == 3, zero, kP)
    sgm = jnp.where(sp == 0, zero, sg)
    first, last = lane == 0, lane == 127

    def along_x(row):
        east = [roll(v, 127, 1) for v in row] + [zero]
        west = [zero] + [roll(v, 1, 1) for v in row]
        return [
            k0 * row[t]
            + kE * jnp.where(last, east[t + 1], east[t])
            + kW * jnp.where(first, west[t], west[t + 1])
            for t in range(NT)
        ]

    def compact(four):
        v = four[0]
        for j in range(1, 4):
            v = jnp.where(sp == j, roll(four[j], j, 0), v)
        return v

    pltpu.make_async_copy(sx, SX, s_sx).wait()

    @pl.loop(0, 8)
    def _(i):
        rows = pl.ds(pl.multiple_of(i * 16, 16), 16)
        SXH[rows, :], SXL[rows, :] = split(SX[rows, :])

    pltpu.make_async_copy(sy, SY, s_sy).wait()
    for b in range(16):
        SYT[b * 128 : (b + 1) * 128, :] = SY[:, b * 128 : (b + 1) * 128].T
    for r in range(ROWS):
        rows = slice(r * 128, (r + 1) * 128)
        SYH[rows, :], SYL[rows, :] = split(SYT[pl.ds(r, 128, stride=16), :])

    def project(read, rows):
        total = jnp.zeros((rows, 128), F32)
        for c in range(NT // 2):
            high, low = split(jnp.concatenate([read(2 * c), read(2 * c + 1)], axis=1))
            cols = slice(c * 256, (c + 1) * 256)
            nt = ((1,), (1,))
            total += dot(high, SXH[:, cols], nt) + dot(low, SXH[:, cols], nt) + dot(high, SXL[:, cols], nt)
        return total

    P0 = project(lambda t: VB[:, t].reshape(32, 128), 32).reshape(4, 8, 128)

    @pl.when(inner)
    def _():
        pl.semaphore_wait(go, 1)

    north = {"gy": gy + 1, "gz": gz}
    south = {"gy": gy - 1, "gz": gz}

    def to_north():
        return remote(F.at[ROWS], F.at[0], ys.at[0], yr.at[0], north)

    def to_south():
        return remote(F.at[1], F.at[ROWS + 1], ys.at[1], yr.at[1], south)

    @pl.when(gy < DEVS - 1)
    def _():
        to_north().start()

    @pl.when(gy > 0)
    def _():
        to_south().start()

    pltpu.make_async_copy(RR, RR, s_rr).wait()
    for f in range(2):
        deck(f).wait_recv()

    @pl.when(gy > 0)
    def _():
        to_north().wait_recv()

    @pl.when(gy < DEVS - 1)
    def _():
        to_south().wait_recv()

    @pl.loop(0, ROWS)
    def _(r):
        row = [F[r + 1, t] for t in range(NT)]
        ahead = along_x(row)
        after = []
        for t in range(NT):
            v = row[t]
            up = jnp.where(sp == 3, HB[r, t], roll(v, 7, 0))
            c = ahead[t] + kN * F[r + 2, t] + kS * F[r, t] + kP * up + kMz * roll(v, 1, 0)
            c += sg * RR[r, t] * v * roll(v, 4, 0)
            CG[0, r, t] = c
            after.append(c)
        for t, g in enumerate(along_x(after)):
            c = after[t]
            CG[1, r, t] = g + sgm * RR[r, t] * c * roll(c, 4, 0)

    early = project(lambda t: CG[:, :, t].reshape(256, 128), 256)
    P1[...] = early[:128].reshape(ROWS, 8, 128)
    for g in range(4):
        PC[g] = compact([P1[4 * g + j] for j in range(4)])

    def to_partner():
        return remote(P1, ZD, zd_s, zd_r, partner)

    def to_opposite():
        return remote(PC, ZC, zc_s, zc_r, opposite)

    to_partner().start()

    @pl.when(inner)
    def _():
        to_opposite().start()

    Q = early[128:].reshape(ROWS, 8, 128)

    @pl.loop(0, 4)
    def _(g):
        for t in range(NT):
            CC[g, t] = compact([CG[0, 4 * g + j, t] for j in range(4)])
            RC[g, t] = compact([RR[4 * g + j, t] for j in range(4)])

    to_partner().wait_recv()
    rows = []
    for r in range(ROWS):
        v = P1[r]
        e = Q[r] + kPz * roll(v, 7, 0) + kMz * roll(v, 1, 0) + jnp.where(sp == 3, kP * ZD[r], zero)
        if r < ROWS - 1:
            e += kN * P1[r + 1]
        if r > 0:
            e += kS * P1[r - 1]
        rows.append(e)
    EA[...] = jnp.concatenate(rows, axis=0).T

    def exchange(src, dst, send, recv):
        @pl.loop(1, DEVS)
        def _(i):
            to = lax.rem(gy + i, DEVS)
            remote(src.at[pl.ds(to, 1), :], dst.at[pl.ds(gy, 1), :], send, recv, {"gy": to, "gz": gz}).start()

        dst[pl.ds(gy, 1), :] = src[pl.ds(gy, 1), :]

    def all_rows(src, dst, send, recv):
        return remote(src.at[pl.ds(0, DEVS - 1), :], dst.at[pl.ds(0, DEVS - 1), :], send, recv, partner)

    exchange(EA, ER, ea_s, ea_r)

    for g in range(4):
        @pl.when(inner)
        def _():
            far(g).wait_recv()

        delta = [kM * UF[g, t] for t in range(NT)]
        for t, q in enumerate(along_x(delta)):
            c = CC[g, t] + delta[t]
            LT[g, t] = delta[t]
            LT[4 + g, t] = q + sg * RC[g, t] * c * roll(c, 4, 0)
    late = project(lambda t: LT[:, t].reshape(64, 128), 64).reshape(8, 8, 128)

    @pl.when(inner)
    def _():
        to_opposite().wait_recv()

    kF = kM * kP * jnp.where(inner, 1.0, 0.0).astype(F32)
    D = [late[g] for g in range(4)]
    X = []
    for g in range(4):
        v = late[4 + g] + kF * P0[g] + kM * ZC[g]
        ahead = roll(D[g + 1], 3, 0) if g < 3 else zero
        behind = roll(D[g - 1], 5, 0) if g > 0 else zero
        v += kN * jnp.where(sp == 3, ahead, roll(D[g], 7, 0))
        v += kS * jnp.where(sp == 0, behind, roll(D[g], 1, 0))
        X.append(v)
    low_edge = kN * P1[0] + jnp.where(sp == 0, kN * D[0], zero)
    high_edge = kS * P1[ROWS - 1] + jnp.where(sp == 0, kS * roll(D[3], 5, 0), zero)
    spare = [low_edge, roll(low_edge, 2, 0), high_edge, roll(high_edge, 2, 0)] + [zero] * (ROWS - 4)
    rows = []
    for r in range(ROWS):
        g, j = divmod(r, 4)
        v = jnp.where(sp == 0, roll(X[g], 8 - j, 0), spare[r])
        rows.append(jnp.where(sp == 1, kM * roll(D[g], 9 - j, 0), v))
    TA[...] = jnp.concatenate(rows, axis=0).T
    exchange(TA, TR, ta_s, ta_r)

    all_rows(EA, ER, ea_s, ea_r).wait_recv()
    AE[...] = ER[...].T
    all_rows(TA, TR, ta_s, ta_r).wait_recv()
    T = TR[...].T
    tail = [T[8 * r : 8 * r + 8] for r in range(ROWS)]
    low_edge = jnp.where(sp >= 2, tail[0], roll(tail[1], 6, 0))
    high_edge = jnp.where(sp >= 2, tail[2], roll(tail[3], 6, 0))
    A = [AE[8 * r : 8 * r + 8, :] + jnp.where(sp < 2, tail[r], zero) for r in range(ROWS)]
    A[ROWS - 1] += jnp.where(last, zero, roll(low_edge, 127, 1))
    A[0] += jnp.where(first, zero, roll(high_edge, 1, 1))
    high, low = split(jnp.concatenate(A, axis=1))
    nn = ((1,), (0,))
    res = dot(high, SYH[...], nn) + dot(low, SYH[...], nn) + dot(high, SYL[...], nn)
    flipped = jnp.where(
        sp == 0, roll(res, 5, 0), jnp.where(sp == 1, roll(res, 7, 0), jnp.where(sp == 2, roll(res, 1, 0), roll(res, 3, 0)))
    )
    res = jnp.where(jnp.full((8, 128), core) == 1, flipped, res)
    out[0, 0] = res[:4]
    out[0, 1] = res[4:]

    @pl.when(inner)
    def _():
        for g in range(4):
            far(g).wait_send()
        to_opposite().wait_send()

    for f in range(2):
        deck(f).wait_send()

    @pl.when(gy < DEVS - 1)
    def _():
        to_north().wait_send()

    @pl.when(gy > 0)
    def _():
        to_south().wait_send()

    to_partner().wait_send()
    all_rows(EA, ER, ea_s, ea_r).wait_send()
    all_rows(TA, TR, ta_s, ta_r).wait_send()


def per_device(fuel, oxidant, rate, velocity, sketch_x, sketch_y):
    def tiles(a):
        return a.reshape(ROWS, 4, NT, 128).transpose(0, 2, 1, 3)

    def tiles4(a):
        return tiles(a).reshape(4, 4, NT, 4, 128)

    vm = lambda *shape, kind=F32: pltpu.VMEM(shape, kind)
    dma, one = pltpu.SemaphoreType.DMA, pltpu.SemaphoreType.REGULAR
    whole = (ROWS, NT, 8, 128)
    plane = (4, NT, 8, 128)
    return pl.pallas_call(
        kernel,
        out_shape=jax.ShapeDtypeStruct((1, 2, 4, 128), F32),
        in_specs=[pl.BlockSpec(memory_space=pl.ANY)] * 5
        + [pl.BlockSpec(memory_space=pltpu.SMEM)]
        + [pl.BlockSpec(memory_space=pl.ANY)] * 2,
        out_specs=pl.BlockSpec(memory_space=pltpu.VMEM),
        scratch_shapes=[
            vm(ROWS + 2, NT, 8, 128), vm(*whole), vm(*whole), vm(*plane), vm(*plane), vm(*plane), vm(*plane),
            vm(2, *whole), vm(8, NT, 8, 128), vm(128, 2048), vm(128, 2048, kind=BF16), vm(128, 2048, kind=BF16),
            vm(128, 2048), vm(2048, 128), vm(2048, 128, kind=BF16), vm(2048, 128, kind=BF16),
            vm(ROWS, 8, 128), vm(ROWS, 8, 128), vm(4, 8, 128), vm(4, 8, 128),
            vm(128, 128), vm(128, 128), vm(128, 128), vm(128, 128), vm(128, 128),
            dma, dma, dma, dma, dma, dma((4,)), dma((4,)), dma((2,)), dma((2,)), dma((2,)), dma((2,)),
            dma, dma, dma, dma, dma, dma, dma, dma,
            one, one, one, one, one, one, one,
        ],
        compiler_params=pltpu.CompilerParams(collective_id=0, has_side_effects=True),
        name="advect_sketch",
    )(tiles(fuel), tiles4(fuel), tiles(oxidant), tiles4(oxidant), tiles(rate), velocity, sketch_x, sketch_y)


def solution(mesh):
    in_specs = (P("gy", "gz", None), P("gy", "gz", None), P("gy", "gz", None), P(), P(), P())
    out_specs = P("gy", None, "gz", None)
    return jax.shard_map(per_device, mesh=mesh, in_specs=in_specs, out_specs=out_specs, check_vma=False)
```

```python
import functools

import jax
import jax.numpy as jnp
from jax import lax
from jax.experimental import pallas as pl
from jax.experimental.pallas import tpu as pltpu
from jax.sharding import PartitionSpec as P

F32, BF16 = jnp.float32, jnp.bfloat16
MESH = pl.DeviceIdType.MESH
NX, NZL, NY = 4, 8, 4
DEVS = NX * NZL * NY
NT = 16
ROWS = 16


def roll(v, shift, axis):
    shift %= v.shape[axis]
    return pltpu.roll(v, shift, axis) if shift else v


def split(v):
    high = v.astype(BF16)
    return high, (v - high.astype(F32)).astype(BF16)


def dot(a, b, dims):
    return lax.dot_general(a, b, (dims, ((), ())), preferred_element_type=F32)


def kernel(
    fuel, fuel4, oxid, oxid4, rate, vel, sx, sy, out,
    F, RR, HB, VB, UF, RC, CC, CG, LT, SX, SXH, SXL, SY, SYT, SYH, SYL,
    P1, ZD, PC, ZC, EA, ER, TA, TR, AE,
    s_vb, s_f, s_rr, s_sx, s_sy, far_s, far_r, ys, yr, ds, dr, zd_s, zd_r, zc_s, zc_r, ea_s, ea_r, ta_s, ta_r,
    zu, zd, go,
):
    gy, gz = lax.axis_index("gy"), lax.axis_index("gz")
    x, zl, y = gy % NX, (gy // NX) % NZL, gy // (NX * NZL)
    core = gz % 2
    inner = (gz == 1) | (gz == 2)
    rim = jnp.logical_not(inner)
    partner = {"gy": gy, "gz": gz + 1 - 2 * core}
    opposite = {"gy": gy, "gz": 3 - gz}

    def at(yy, zz, xx):
        return {"gy": (yy * NZL + zz) * NX + xx, "gz": gz}

    def signal(sem, device):
        pl.semaphore_signal(sem, inc=1, device_id=device, device_id_type=MESH)

    def remote(src, dst, send, recv, device):
        return pltpu.make_async_remote_copy(
            src_ref=src, dst_ref=dst, send_sem=send, recv_sem=recv, device_id=device, device_id_type=MESH
        )

    def plane(p):
        return p + core * (3 - 2 * p)

    for f, src in enumerate((fuel4, oxid4)):
        for j in range(4):
            pltpu.make_async_copy(src.at[:, j, :, plane(0), :], VB.at[:, :, f * 4 + j, :], s_vb).start()
    barrier = pltpu.get_barrier_semaphore()
    above, below = at(y, zl + 1, x), at(y, zl - 1, x)
    rim_gz = 3 * (gz // 2)

    for a in range(NY):
        for b in range(NX):
            device = {"gy": (((y + a) % NY) * NZL + zl) * NX + (x + b) % NX, "gz": rim_gz}
            if a or b:
                signal(barrier, device)

    signal(barrier, partner)

    @pl.when(inner)
    def _():
        signal(barrier, opposite)

    @pl.when(rim)
    def _():
        @pl.when(zl < NZL - 1)
        def _():
            signal(barrier, above)

        @pl.when(zl > 0)
        def _():
            signal(barrier, below)

        UF[...] = jnp.zeros_like(UF)
        ZC[...] = jnp.zeros_like(ZC)

    @pl.when(gy == 0)
    def _():
        F[0] = jnp.zeros((NT, 8, 128), F32)

    @pl.when(gy == DEVS - 1)
    def _():
        F[ROWS + 1] = jnp.zeros((NT, 8, 128), F32)

    pltpu.make_async_copy(VB, VB, s_vb).wait()
    for f, src in enumerate((fuel, oxid)):
        for p in (3, 0, 1, 2):
            pltpu.make_async_copy(src.at[:, :, plane(p), :], F.at[pl.ds(1, ROWS), :, f * 4 + p, :], s_f).start()
    for p in range(4):
        for f in range(2):
            pltpu.make_async_copy(rate.at[:, :, plane(p), :], RR.at[:, :, f * 4 + p, :], s_rr).start()
    pltpu.make_async_copy(sx, SX, s_sx).start()
    pltpu.make_async_copy(sy, SY, s_sy).start()

    @pl.when(inner)
    def _():
        pl.semaphore_wait(barrier, 2)

    @pl.when(rim & ((zl == 0) | (zl == NZL - 1)))
    def _():
        pl.semaphore_wait(barrier, 32)

    @pl.when(rim & (zl > 0) & (zl < NZL - 1))
    def _():
        pl.semaphore_wait(barrier, 33)

    def far(g):
        return remote(VB.at[g], UF.at[g], far_s.at[g], far_r.at[g], opposite)

    @pl.when(inner)
    def _():
        for g in range(4):
            far(g).start()

    def deck(f):
        return remote(
            F.at[pl.ds(1, ROWS), :, f * 4 + 3, :], HB.at[:, :, f * 4 + 3, :], ds.at[f], dr.at[f], partner
        )

    pltpu.make_async_copy(F.at[pl.ds(1, ROWS)], F.at[pl.ds(1, ROWS)], s_f).wait()
    for f in range(2):
        deck(f).start()

    @pl.when(rim)
    def _():
        @pl.when(zl == 0)
        def _():
            signal(zu, above)

        @pl.when(zl == NZL - 1)
        def _():
            signal(zd, below)

        @pl.when((zl > 0) & (zl < NZL // 2))
        def _():
            pl.semaphore_wait(zu, 1)
            signal(zu, above)
            pl.semaphore_wait(zd, 1)
            signal(zd, below)

        @pl.when((zl < NZL - 1) & (zl >= NZL // 2))
        def _():
            pl.semaphore_wait(zd, 1)
            signal(zd, below)
            pl.semaphore_wait(zu, 1)
            signal(zu, above)

        @pl.when(zl == 0)
        def _():
            pl.semaphore_wait(zd, 1)

        @pl.when(zl == NZL - 1)
        def _():
            pl.semaphore_wait(zu, 1)

        signal(go, partner)

    north = {"gy": gy + 1, "gz": gz}
    south = {"gy": gy - 1, "gz": gz}

    def to_north():
        return remote(F.at[ROWS], F.at[0], ys.at[0], yr.at[0], north)

    def to_south():
        return remote(F.at[1], F.at[ROWS + 1], ys.at[1], yr.at[1], south)

    def send_rows():
        @pl.when(gy < DEVS - 1)
        def _():
            to_north().start()

        @pl.when(gy > 0)
        def _():
            to_south().start()

    @pl.when(gz == 1)
    def _():
        pl.semaphore_wait(go, 1)

    @pl.when(gz != 2)
    def _():
        send_rows()

    sub = lax.broadcasted_iota(jnp.int32, (8, 128), 0)
    lane = lax.broadcasted_iota(jnp.int32, (8, 128), 1)
    sp = sub % 4
    v0, v1 = 0.5 * vel[0], 0.5 * vel[1]
    v2 = 0.5 * vel[2] * (1 - 2 * core).astype(F32)
    alpha = jnp.where(sub < 4, 0.1, 0.05).astype(F32)
    zero = jnp.zeros((8, 128), F32)
    k0, kE, kW, kN, kS = 1.0 - 6.0 * alpha, alpha - v0, alpha + v0, alpha - v1, alpha + v1
    kP, kM = alpha - v2, alpha + v2
    sg = jnp.where(sub < 4, -1.0, 1.0).astype(F32)
    kMz = jnp.where(sp == 0, zero, kM)
    kPz = jnp.where(sp == 3, zero, kP)
    sgm = jnp.where(sp == 0, zero, sg)
    first, last = lane == 0, lane == 127

    def along_x(row):
        east = [roll(v, 127, 1) for v in row] + [zero]
        west = [zero] + [roll(v, 1, 1) for v in row]
        return [
            k0 * row[t]
            + kE * jnp.where(last, east[t + 1], east[t])
            + kW * jnp.where(first, west[t], west[t + 1])
            for t in range(NT)
        ]

    def compact(four):
        v = four[0]
        for j in range(1, 4):
            v = jnp.where(sp == j, roll(four[j], j, 0), v)
        return v

    pltpu.make_async_copy(sx, SX, s_sx).wait()

    @pl.loop(0, 8)
    def _(i):
        rows = pl.ds(pl.multiple_of(i * 16, 16), 16)
        SXH[rows, :], SXL[rows, :] = split(SX[rows, :])

    pltpu.make_async_copy(sy, SY, s_sy).wait()
    for b in range(16):
        SYT[b * 128 : (b + 1) * 128, :] = SY[:, b * 128 : (b + 1) * 128].T
    for r in range(ROWS):
        rows = slice(r * 128, (r + 1) * 128)
        SYH[rows, :], SYL[rows, :] = split(SYT[pl.ds(r, 128, stride=16), :])

    def project(read, rows):
        total = jnp.zeros((rows, 128), F32)
        for c in range(NT // 2):
            high, low = split(jnp.concatenate([read(2 * c), read(2 * c + 1)], axis=1))
            cols = slice(c * 256, (c + 1) * 256)
            nt = ((1,), (1,))
            total += dot(high, SXH[:, cols], nt) + dot(low, SXH[:, cols], nt) + dot(high, SXL[:, cols], nt)
        return total

    pltpu.make_async_copy(RR, RR, s_rr).wait()
    for f in range(2):
        deck(f).wait_recv()

    @pl.loop(0, ROWS)
    def _(r):
        kn, ks = jnp.where(r == ROWS - 1, zero, kN), jnp.where(r == 0, zero, kS)
        rn, rs = jnp.minimum(r + 2, ROWS), jnp.maximum(r, 1)
        row = [F[r + 1, t] for t in range(NT)]
        ahead = along_x(row)
        after = []
        for t in range(NT):
            v = row[t]
            up = jnp.where(sp == 3, HB[r, t], roll(v, 7, 0))
            c = ahead[t] + kn * F[rn, t] + ks * F[rs, t] + kP * up + kMz * roll(v, 1, 0)
            c += sg * RR[r, t] * v * roll(v, 4, 0)
            CG[0, r, t] = c
            after.append(c)
        for t, g in enumerate(along_x(after)):
            c = after[t]
            CG[1, r, t] = g + sgm * RR[r, t] * c * roll(c, 4, 0)

    def to_partner():
        return remote(P1, ZD, zd_s, zd_r, partner)

    def to_opposite():
        return remote(PC, ZC, zc_s, zc_r, opposite)

    def compact_rows(g):
        for t in range(NT):
            CC[g, t] = compact([CG[0, 4 * g + j, t] for j in range(4)])

    @pl.loop(0, 4)
    def _(g):
        compact_rows(g)
        for t in range(NT):
            RC[g, t] = compact([RR[4 * g + j, t] for j in range(4)])

    local = project(lambda t: jnp.concatenate([VB[:, t].reshape(32, 128), CC[:, t].reshape(32, 128)], axis=0), 64)
    P0 = local[:32].reshape(4, 8, 128)
    PC[...] = local[32:].reshape(4, 8, 128)

    @pl.when(inner)
    def _():
        to_opposite().start()

    @pl.when(gz == 2)
    def _():
        pl.semaphore_wait(go, 1)
        send_rows()

    @pl.when(gy > 0)
    def _():
        to_north().wait_recv()

    @pl.when(gy < DEVS - 1)
    def _():
        to_south().wait_recv()

    for r, halo, k in ((0, 0, kS), (ROWS - 1, ROWS + 1, kN)):
        after = [CG[0, r, t] + k * F[halo, t] for t in range(NT)]
        for t, g in enumerate(along_x(after)):
            c = after[t]
            CG[0, r, t] = c
            CG[1, r, t] = g + sgm * RR[r, t] * c * roll(c, 4, 0)
    compact_rows(0)
    compact_rows(3)

    early = project(lambda t: CG[:, :, t].reshape(256, 128), 256)
    P1[...] = early[:128].reshape(ROWS, 8, 128)
    to_partner().start()
    Q = early[128:].reshape(ROWS, 8, 128)

    to_partner().wait_recv()
    rows = []
    for r in range(ROWS):
        v = P1[r]
        e = Q[r] + kPz * roll(v, 7, 0) + kMz * roll(v, 1, 0) + jnp.where(sp == 3, kP * ZD[r], zero)
        if r < ROWS - 1:
            e += kN * P1[r + 1]
        if r > 0:
            e += kS * P1[r - 1]
        rows.append(e)
    EA[...] = jnp.concatenate(rows, axis=0).T

    def exchange(src, dst, send, recv):
        def one(to):
            remote(src.at[pl.ds(to, 1), :], dst.at[pl.ds(gy, 1), :], send, recv, {"gy": to, "gz": gz}).start()

        @pl.loop(0, NZL)
        def _(n):
            zz = jnp.where(zl < NZL // 2, NZL - 1 - n, n)
            for m in range(1, NX * NY):
                one((((y + m // NX) % NY) * NZL + zz) * NX + (x + m % NX) % NX)

            @pl.when(zz != zl)
            def _():
                one((y * NZL + zz) * NX + x)

        dst[pl.ds(gy, 1), :] = src[pl.ds(gy, 1), :]

    def all_rows(src, dst, send, recv):
        return remote(src.at[pl.ds(0, DEVS - 1), :], dst.at[pl.ds(0, DEVS - 1), :], send, recv, partner)

    exchange(EA, ER, ea_s, ea_r)

    for g in range(4):
        @pl.when(inner)
        def _():
            far(g).wait_recv()

        delta = [kM * UF[g, t] for t in range(NT)]
        for t, q in enumerate(along_x(delta)):
            c = CC[g, t] + delta[t]
            LT[g, t] = delta[t]
            LT[4 + g, t] = q + sg * RC[g, t] * c * roll(c, 4, 0)
    late = project(lambda t: LT[:, t].reshape(64, 128), 64).reshape(8, 8, 128)

    @pl.when(inner)
    def _():
        to_opposite().wait_recv()

    kF = kM * kP * jnp.where(inner, 1.0, 0.0).astype(F32)
    D = [late[g] for g in range(4)]
    X = []
    for g in range(4):
        v = late[4 + g] + kF * P0[g] + kM * ZC[g]
        ahead = roll(D[g + 1], 3, 0) if g < 3 else zero
        behind = roll(D[g - 1], 5, 0) if g > 0 else zero
        v += kN * jnp.where(sp == 3, ahead, roll(D[g], 7, 0))
        v += kS * jnp.where(sp == 0, behind, roll(D[g], 1, 0))
        X.append(v)
    low_edge = kN * P1[0] + jnp.where(sp == 0, 2.0 * kN * D[0], zero)
    high_edge = kS * P1[ROWS - 1] + jnp.where(sp == 0, 2.0 * kS * roll(D[3], 5, 0), zero)
    spare = [low_edge, roll(low_edge, 2, 0), high_edge, roll(high_edge, 2, 0)] + [zero] * (ROWS - 4)
    rows = []
    for r in range(ROWS):
        g, j = divmod(r, 4)
        v = jnp.where(sp == 0, roll(X[g], 8 - j, 0), spare[r])
        rows.append(jnp.where(sp == 1, kM * roll(D[g], 9 - j, 0), v))
    TA[...] = jnp.concatenate(rows, axis=0).T
    exchange(TA, TR, ta_s, ta_r)

    all_rows(EA, ER, ea_s, ea_r).wait_recv()
    AE[...] = ER[...].T
    all_rows(TA, TR, ta_s, ta_r).wait_recv()
    T = TR[...].T
    tail = [T[8 * r : 8 * r + 8] for r in range(ROWS)]
    low_edge = jnp.where(sp >= 2, tail[0], roll(tail[1], 6, 0))
    high_edge = jnp.where(sp >= 2, tail[2], roll(tail[3], 6, 0))
    A = [AE[8 * r : 8 * r + 8, :] + jnp.where(sp < 2, tail[r], zero) for r in range(ROWS)]
    A[ROWS - 1] += jnp.where(last, zero, roll(low_edge, 127, 1))
    A[0] += jnp.where(first, zero, roll(high_edge, 1, 1))
    high, low = split(jnp.concatenate(A, axis=1))
    nn = ((1,), (0,))
    res = dot(high, SYH[...], nn) + dot(low, SYH[...], nn) + dot(high, SYL[...], nn)
    flipped = jnp.where(
        sp == 0, roll(res, 5, 0), jnp.where(sp == 1, roll(res, 7, 0), jnp.where(sp == 2, roll(res, 1, 0), roll(res, 3, 0)))
    )
    res = jnp.where(jnp.full((8, 128), core) == 1, flipped, res)
    out[0, 0] = res[:4]
    out[0, 1] = res[4:]

    @pl.when(inner)
    def _():
        for g in range(4):
            far(g).wait_send()
        to_opposite().wait_send()

    for f in range(2):
        deck(f).wait_send()

    @pl.when(gy < DEVS - 1)
    def _():
        to_north().wait_send()

    @pl.when(gy > 0)
    def _():
        to_south().wait_send()

    to_partner().wait_send()
    all_rows(EA, ER, ea_s, ea_r).wait_send()
    all_rows(TA, TR, ta_s, ta_r).wait_send()


def per_device(fuel, oxidant, rate, velocity, sketch_x, sketch_y):
    def tiles(a):
        return a.reshape(ROWS, 4, NT, 128).transpose(0, 2, 1, 3)

    def tiles4(a):
        return tiles(a).reshape(4, 4, NT, 4, 128)

    vm = lambda *shape, kind=F32: pltpu.VMEM(shape, kind)
    dma, one = pltpu.SemaphoreType.DMA, pltpu.SemaphoreType.REGULAR
    whole = (ROWS, NT, 8, 128)
    plane = (4, NT, 8, 128)
    return pl.pallas_call(
        kernel,
        out_shape=jax.ShapeDtypeStruct((1, 2, 4, 128), F32),
        in_specs=[pl.BlockSpec(memory_space=pl.ANY)] * 5
        + [pl.BlockSpec(memory_space=pltpu.SMEM)]
        + [pl.BlockSpec(memory_space=pl.ANY)] * 2,
        out_specs=pl.BlockSpec(memory_space=pltpu.VMEM),
        scratch_shapes=[
            vm(ROWS + 2, NT, 8, 128), vm(*whole), vm(*whole), vm(*plane), vm(*plane), vm(*plane), vm(*plane),
            vm(2, *whole), vm(8, NT, 8, 128), vm(128, 2048), vm(128, 2048, kind=BF16), vm(128, 2048, kind=BF16),
            vm(128, 2048), vm(2048, 128), vm(2048, 128, kind=BF16), vm(2048, 128, kind=BF16),
            vm(ROWS, 8, 128), vm(ROWS, 8, 128), vm(4, 8, 128), vm(4, 8, 128),
            vm(128, 128), vm(128, 128), vm(128, 128), vm(128, 128), vm(128, 128),
            dma, dma, dma, dma, dma, dma((4,)), dma((4,)), dma((2,)), dma((2,)), dma((2,)), dma((2,)),
            dma, dma, dma, dma, dma, dma, dma, dma,
            one, one, one,
        ],
        compiler_params=pltpu.CompilerParams(collective_id=0, has_side_effects=True),
        name="advect_sketch",
    )(tiles(fuel), tiles4(fuel), tiles(oxidant), tiles4(oxidant), tiles(rate), velocity, sketch_x, sketch_y)


def solution(mesh):
    in_specs = (P("gy", "gz", None), P("gy", "gz", None), P("gy", "gz", None), P(), P(), P())
    out_specs = P("gy", None, "gz", None)
    return jax.shard_map(per_device, mesh=mesh, in_specs=in_specs, out_specs=out_specs, check_vma=False)
```

```python
import functools

import jax
import jax.numpy as jnp
from jax import lax
from jax.experimental import pallas as pl
from jax.experimental.pallas import tpu as pltpu
from jax.sharding import PartitionSpec as P

F32, BF16 = jnp.float32, jnp.bfloat16
MESH = pl.DeviceIdType.MESH
NX, NZL, NY = 4, 8, 4
DEVS = NX * NZL * NY
NT = 16
ROWS = 16


def roll(v, shift, axis):
    shift %= v.shape[axis]
    return pltpu.roll(v, shift, axis) if shift else v


def split(v):
    high = v.astype(BF16)
    return high, (v - high.astype(F32)).astype(BF16)


def dot(a, b, dims):
    return lax.dot_general(a, b, (dims, ((), ())), preferred_element_type=F32)


def kernel(
    fuel, fuel4, oxid, oxid4, rate, vel, sx, sy, out,
    F, RR, HB, VB, UF, RC, CC, CG, LT, SX, SXH, SXL, SY, SYT, SYH, SYL,
    P1, ZD, PC, ZC, EA, ER, TA, TR, AE,
    s_vb, s_f, s_rr, s_sx, s_sy, far_s, far_r, ys, yr, ds, dr, zd_s, zd_r, zc_s, zc_r, ea_s, ea_r, ta_s, ta_r,
    zu, zd, go, near, ready,
):
    gy, gz = lax.axis_index("gy"), lax.axis_index("gz")
    x, zl, y = gy % NX, (gy // NX) % NZL, gy // (NX * NZL)
    core = gz % 2
    inner = (gz == 1) | (gz == 2)
    rim = jnp.logical_not(inner)
    partner = {"gy": gy, "gz": gz + 1 - 2 * core}
    opposite = {"gy": gy, "gz": 3 - gz}

    def at(yy, zz, xx):
        return {"gy": (yy * NZL + zz) * NX + xx, "gz": gz}

    def signal(sem, device):
        pl.semaphore_signal(sem, inc=1, device_id=device, device_id_type=MESH)

    def remote(src, dst, send, recv, device):
        return pltpu.make_async_remote_copy(
            src_ref=src, dst_ref=dst, send_sem=send, recv_sem=recv, device_id=device, device_id_type=MESH
        )

    def plane(p):
        return p + core * (3 - 2 * p)

    for f, src in enumerate((fuel4, oxid4)):
        for j in range(4):
            pltpu.make_async_copy(src.at[:, j, :, plane(0), :], VB.at[:, :, f * 4 + j, :], s_vb).start()
    barrier = pltpu.get_barrier_semaphore()
    above, below = at(y, zl + 1, x), at(y, zl - 1, x)
    rim_gz = 3 * (gz // 2)

    for a in range(NY):
        for b in range(NX):
            device = {"gy": (((y + a) % NY) * NZL + zl) * NX + (x + b) % NX, "gz": rim_gz}
            if a or b:
                signal(barrier, device)

    signal(barrier, partner)

    @pl.when((x == NX - 1) & (gy < DEVS - 1))
    def _():
        signal(barrier, {"gy": gy + 1, "gz": rim_gz})

    @pl.when((x == 0) & (gy > 0))
    def _():
        signal(barrier, {"gy": gy - 1, "gz": rim_gz})

    @pl.when(gz == 1)
    def _():
        signal(barrier, opposite)

    @pl.when(rim)
    def _():
        @pl.when(zl < NZL - 1)
        def _():
            signal(barrier, above)

        @pl.when(zl > 0)
        def _():
            signal(barrier, below)

        UF[...] = jnp.zeros_like(UF)
        ZC[...] = jnp.zeros_like(ZC)

    @pl.when(gy == 0)
    def _():
        F[0] = jnp.zeros((NT, 8, 128), F32)

    @pl.when(gy == DEVS - 1)
    def _():
        F[ROWS + 1] = jnp.zeros((NT, 8, 128), F32)

    pltpu.make_async_copy(VB, VB, s_vb).wait()
    for f, src in enumerate((fuel, oxid)):
        for p in (3, 0, 1, 2):
            pltpu.make_async_copy(src.at[:, :, plane(p), :], F.at[pl.ds(1, ROWS), :, f * 4 + p, :], s_f).start()
    for p in range(4):
        for f in range(2):
            pltpu.make_async_copy(rate.at[:, :, plane(p), :], RR.at[:, :, f * 4 + p, :], s_rr).start()
    pltpu.make_async_copy(sx, SX, s_sx).start()
    pltpu.make_async_copy(sy, SY, s_sy).start()

    @pl.when(gz == 1)
    def _():
        pl.semaphore_wait(barrier, 1)

    @pl.when(gz == 2)
    def _():
        pl.semaphore_wait(barrier, 2)
        signal(ready, opposite)

    ends = jnp.where((zl == 0) | (zl == NZL - 1), 32, 33)
    ends += jnp.where((x == 0) & (gy > 0), 2, 0) + jnp.where((x == NX - 1) & (gy < DEVS - 1), 2, 0)

    @pl.when(rim)
    def _():
        pl.semaphore_wait(barrier, ends)
        signal(near, partner)

    def far(g):
        return remote(VB.at[g], UF.at[g], far_s.at[g], far_r.at[g], opposite)

    @pl.when(gz == 2)
    def _():
        for g in range(4):
            far(g).start()

    def deck(f):
        return remote(
            F.at[pl.ds(1, ROWS), :, f * 4 + 3, :], HB.at[:, :, f * 4 + 3, :], ds.at[f], dr.at[f], partner
        )

    pltpu.make_async_copy(F.at[pl.ds(1, ROWS)], F.at[pl.ds(1, ROWS)], s_f).wait()
    for f in range(2):
        deck(f).start()

    north = {"gy": gy + 1, "gz": gz}
    south = {"gy": gy - 1, "gz": gz}

    def to_north():
        return remote(F.at[ROWS], F.at[0], ys.at[0], yr.at[0], north)

    def to_south():
        return remote(F.at[1], F.at[ROWS + 1], ys.at[1], yr.at[1], south)

    def send_rows():
        @pl.when(gy < DEVS - 1)
        def _():
            to_north().start()

        @pl.when(gy > 0)
        def _():
            to_south().start()

    @pl.when(gz == 1)
    def _():
        pl.semaphore_wait(near, 1)

    @pl.when(gz != 2)
    def _():
        send_rows()

    sub = lax.broadcasted_iota(jnp.int32, (8, 128), 0)
    lane = lax.broadcasted_iota(jnp.int32, (8, 128), 1)
    sp = sub % 4
    v0, v1 = 0.5 * vel[0], 0.5 * vel[1]
    v2 = 0.5 * vel[2] * (1 - 2 * core).astype(F32)
    alpha = jnp.where(sub < 4, 0.1, 0.05).astype(F32)
    zero = jnp.zeros((8, 128), F32)
    k0, kE, kW, kN, kS = 1.0 - 6.0 * alpha, alpha - v0, alpha + v0, alpha - v1, alpha + v1
    kP, kM = alpha - v2, alpha + v2
    sg = jnp.where(sub < 4, -1.0, 1.0).astype(F32)
    kMz = jnp.where(sp == 0, zero, kM)
    kPz = jnp.where(sp == 3, zero, kP)
    sgm = jnp.where(sp == 0, zero, sg)
    first, last = lane == 0, lane == 127

    def along_x(row):
        east = [roll(v, 127, 1) for v in row] + [zero]
        west = [zero] + [roll(v, 1, 1) for v in row]
        return [
            k0 * row[t]
            + kE * jnp.where(last, east[t + 1], east[t])
            + kW * jnp.where(first, west[t], west[t + 1])
            for t in range(NT)
        ]

    def compact(four):
        v = four[0]
        for j in range(1, 4):
            v = jnp.where(sp == j, roll(four[j], j, 0), v)
        return v

    pltpu.make_async_copy(sx, SX, s_sx).wait()

    @pl.loop(0, 8)
    def _(i):
        rows = pl.ds(pl.multiple_of(i * 16, 16), 16)
        SXH[rows, :], SXL[rows, :] = split(SX[rows, :])

    pltpu.make_async_copy(sy, SY, s_sy).wait()
    for b in range(16):
        SYT[b * 128 : (b + 1) * 128, :] = SY[:, b * 128 : (b + 1) * 128].T
    for r in range(ROWS):
        rows = slice(r * 128, (r + 1) * 128)
        SYH[rows, :], SYL[rows, :] = split(SYT[pl.ds(r, 128, stride=16), :])

    def project(read, rows):
        total = jnp.zeros((rows, 128), F32)
        for c in range(NT // 2):
            high, low = split(jnp.concatenate([read(2 * c), read(2 * c + 1)], axis=1))
            cols = slice(c * 256, (c + 1) * 256)
            nt = ((1,), (1,))
            total += dot(high, SXH[:, cols], nt) + dot(low, SXH[:, cols], nt) + dot(high, SXL[:, cols], nt)
        return total

    pltpu.make_async_copy(RR, RR, s_rr).wait()
    for f in range(2):
        deck(f).wait_recv()

    @pl.loop(0, ROWS)
    def _(r):
        kn, ks = jnp.where(r == ROWS - 1, zero, kN), jnp.where(r == 0, zero, kS)
        rn, rs = jnp.minimum(r + 2, ROWS), jnp.maximum(r, 1)
        row = [F[r + 1, t] for t in range(NT)]
        ahead = along_x(row)
        after = []
        for t in range(NT):
            v = row[t]
            up = jnp.where(sp == 3, HB[r, t], roll(v, 7, 0))
            c = ahead[t] + kn * F[rn, t] + ks * F[rs, t] + kP * up + kMz * roll(v, 1, 0)
            c += sg * RR[r, t] * v * roll(v, 4, 0)
            CG[0, r, t] = c
            after.append(c)
        for t, g in enumerate(along_x(after)):
            c = after[t]
            CG[1, r, t] = g + sgm * RR[r, t] * c * roll(c, 4, 0)

    def to_partner():
        return remote(P1, ZD, zd_s, zd_r, partner)

    def to_opposite():
        return remote(PC, ZC, zc_s, zc_r, opposite)

    def compact_rows(g):
        for t in range(NT):
            CC[g, t] = compact([CG[0, 4 * g + j, t] for j in range(4)])

    @pl.loop(0, 4)
    def _(g):
        compact_rows(g)
        for t in range(NT):
            RC[g, t] = compact([RR[4 * g + j, t] for j in range(4)])

    local = project(lambda t: jnp.concatenate([VB[:, t].reshape(32, 128), CC[:, t].reshape(32, 128)], axis=0), 64)
    P0 = local[:32].reshape(4, 8, 128)
    PC[...] = local[32:].reshape(4, 8, 128)

    @pl.when(gz == 1)
    def _():
        pl.semaphore_wait(ready, 1)
        for g in range(4):
            far(g).start()

    @pl.when(inner)
    def _():
        to_opposite().start()

    @pl.when(gz == 2)
    def _():
        pl.semaphore_wait(near, 1)
        send_rows()

    @pl.when(rim)
    def _():
        @pl.when(zl == 0)
        def _():
            signal(zu, above)

        @pl.when(zl == NZL - 1)
        def _():
            signal(zd, below)

        @pl.when((zl > 0) & (zl < NZL // 2))
        def _():
            pl.semaphore_wait(zu, 1)
            signal(zu, above)
            pl.semaphore_wait(zd, 1)
            signal(zd, below)

        @pl.when((zl < NZL - 1) & (zl >= NZL // 2))
        def _():
            pl.semaphore_wait(zd, 1)
            signal(zd, below)
            pl.semaphore_wait(zu, 1)
            signal(zu, above)

        @pl.when(zl == 0)
        def _():
            pl.semaphore_wait(zd, 1)

        @pl.when(zl == NZL - 1)
        def _():
            pl.semaphore_wait(zu, 1)

        signal(go, partner)

    @pl.when(gy > 0)
    def _():
        to_north().wait_recv()

    @pl.when(gy < DEVS - 1)
    def _():
        to_south().wait_recv()

    for r, halo, k in ((0, 0, kS), (ROWS - 1, ROWS + 1, kN)):
        after = [CG[0, r, t] + k * F[halo, t] for t in range(NT)]
        for t, g in enumerate(along_x(after)):
            c = after[t]
            CG[0, r, t] = c
            CG[1, r, t] = g + sgm * RR[r, t] * c * roll(c, 4, 0)
    compact_rows(0)
    compact_rows(3)

    early = project(lambda t: CG[:, :, t].reshape(256, 128), 256)
    P1[...] = early[:128].reshape(ROWS, 8, 128)
    to_partner().start()
    Q = early[128:].reshape(ROWS, 8, 128)

    to_partner().wait_recv()
    rows = []
    for r in range(ROWS):
        v = P1[r]
        e = Q[r] + kPz * roll(v, 7, 0) + kMz * roll(v, 1, 0) + jnp.where(sp == 3, kP * ZD[r], zero)
        if r < ROWS - 1:
            e += kN * P1[r + 1]
        if r > 0:
            e += kS * P1[r - 1]
        rows.append(e)
    EA[...] = jnp.concatenate(rows, axis=0).T

    def exchange(src, dst, send, recv):
        def one(to):
            remote(src.at[pl.ds(to, 1), :], dst.at[pl.ds(gy, 1), :], send, recv, {"gy": to, "gz": gz}).start()

        @pl.loop(0, NZL)
        def _(n):
            zz = jnp.where(zl < NZL // 2, NZL - 1 - n, n)
            for m in range(1, NX * NY):
                one((((y + m // NX) % NY) * NZL + zz) * NX + (x + m % NX) % NX)

            @pl.when(zz != zl)
            def _():
                one((y * NZL + zz) * NX + x)

        dst[pl.ds(gy, 1), :] = src[pl.ds(gy, 1), :]

    def all_rows(src, dst, send, recv):
        return remote(src.at[pl.ds(0, DEVS - 1), :], dst.at[pl.ds(0, DEVS - 1), :], send, recv, partner)

    @pl.when(inner)
    def _():
        pl.semaphore_wait(go, 1)

    exchange(EA, ER, ea_s, ea_r)

    for g in range(4):
        @pl.when(inner)
        def _():
            far(g).wait_recv()

        delta = [kM * UF[g, t] for t in range(NT)]
        for t, q in enumerate(along_x(delta)):
            c = CC[g, t] + delta[t]
            LT[g, t] = delta[t]
            LT[4 + g, t] = q + sg * RC[g, t] * c * roll(c, 4, 0)
    late = project(lambda t: LT[:, t].reshape(64, 128), 64).reshape(8, 8, 128)

    @pl.when(inner)
    def _():
        to_opposite().wait_recv()

    kF = kM * kP * jnp.where(inner, 1.0, 0.0).astype(F32)
    D = [late[g] for g in range(4)]
    X = []
    for g in range(4):
        v = late[4 + g] + kF * P0[g] + kM * ZC[g]
        ahead = roll(D[g + 1], 3, 0) if g < 3 else zero
        behind = roll(D[g - 1], 5, 0) if g > 0 else zero
        v += kN * jnp.where(sp == 3, ahead, roll(D[g], 7, 0))
        v += kS * jnp.where(sp == 0, behind, roll(D[g], 1, 0))
        X.append(v)
    low_edge = kN * P1[0] + jnp.where(sp == 0, 2.0 * kN * D[0], zero)
    high_edge = kS * P1[ROWS - 1] + jnp.where(sp == 0, 2.0 * kS * roll(D[3], 5, 0), zero)
    spare = [low_edge, roll(low_edge, 2, 0), high_edge, roll(high_edge, 2, 0)] + [zero] * (ROWS - 4)
    rows = []
    for r in range(ROWS):
        g, j = divmod(r, 4)
        v = jnp.where(sp == 0, roll(X[g], 8 - j, 0), spare[r])
        rows.append(jnp.where(sp == 1, kM * roll(D[g], 9 - j, 0), v))
    TA[...] = jnp.concatenate(rows, axis=0).T
    exchange(TA, TR, ta_s, ta_r)

    all_rows(EA, ER, ea_s, ea_r).wait_recv()
    AE[...] = ER[...].T
    all_rows(TA, TR, ta_s, ta_r).wait_recv()
    T = TR[...].T
    tail = [T[8 * r : 8 * r + 8] for r in range(ROWS)]
    low_edge = jnp.where(sp >= 2, tail[0], roll(tail[1], 6, 0))
    high_edge = jnp.where(sp >= 2, tail[2], roll(tail[3], 6, 0))
    A = [AE[8 * r : 8 * r + 8, :] + jnp.where(sp < 2, tail[r], zero) for r in range(ROWS)]
    A[ROWS - 1] += jnp.where(last, zero, roll(low_edge, 127, 1))
    A[0] += jnp.where(first, zero, roll(high_edge, 1, 1))
    high, low = split(jnp.concatenate(A, axis=1))
    nn = ((1,), (0,))
    res = dot(high, SYH[...], nn) + dot(low, SYH[...], nn) + dot(high, SYL[...], nn)
    flipped = jnp.where(
        sp == 0, roll(res, 5, 0), jnp.where(sp == 1, roll(res, 7, 0), jnp.where(sp == 2, roll(res, 1, 0), roll(res, 3, 0)))
    )
    res = jnp.where(jnp.full((8, 128), core) == 1, flipped, res)
    out[0, 0] = res[:4]
    out[0, 1] = res[4:]

    @pl.when(inner)
    def _():
        for g in range(4):
            far(g).wait_send()
        to_opposite().wait_send()

    for f in range(2):
        deck(f).wait_send()

    @pl.when(gy < DEVS - 1)
    def _():
        to_north().wait_send()

    @pl.when(gy > 0)
    def _():
        to_south().wait_send()

    to_partner().wait_send()
    all_rows(EA, ER, ea_s, ea_r).wait_send()
    all_rows(TA, TR, ta_s, ta_r).wait_send()


def per_device(fuel, oxidant, rate, velocity, sketch_x, sketch_y):
    def tiles(a):
        return a.reshape(ROWS, 4, NT, 128).transpose(0, 2, 1, 3)

    def tiles4(a):
        return tiles(a).reshape(4, 4, NT, 4, 128)

    vm = lambda *shape, kind=F32: pltpu.VMEM(shape, kind)
    dma, one = pltpu.SemaphoreType.DMA, pltpu.SemaphoreType.REGULAR
    whole = (ROWS, NT, 8, 128)
    plane = (4, NT, 8, 128)
    return pl.pallas_call(
        kernel,
        out_shape=jax.ShapeDtypeStruct((1, 2, 4, 128), F32),
        in_specs=[pl.BlockSpec(memory_space=pl.ANY)] * 5
        + [pl.BlockSpec(memory_space=pltpu.SMEM)]
        + [pl.BlockSpec(memory_space=pl.ANY)] * 2,
        out_specs=pl.BlockSpec(memory_space=pltpu.VMEM),
        scratch_shapes=[
            vm(ROWS + 2, NT, 8, 128), vm(*whole), vm(*whole), vm(*plane), vm(*plane), vm(*plane), vm(*plane),
            vm(2, *whole), vm(8, NT, 8, 128), vm(128, 2048), vm(128, 2048, kind=BF16), vm(128, 2048, kind=BF16),
            vm(128, 2048), vm(2048, 128), vm(2048, 128, kind=BF16), vm(2048, 128, kind=BF16),
            vm(ROWS, 8, 128), vm(ROWS, 8, 128), vm(4, 8, 128), vm(4, 8, 128),
            vm(128, 128), vm(128, 128), vm(128, 128), vm(128, 128), vm(128, 128),
            dma, dma, dma, dma, dma, dma((4,)), dma((4,)), dma((2,)), dma((2,)), dma((2,)), dma((2,)),
            dma, dma, dma, dma, dma, dma, dma, dma,
            one, one, one, one, one,
        ],
        compiler_params=pltpu.CompilerParams(collective_id=0, has_side_effects=True),
        name="advect_sketch",
    )(tiles(fuel), tiles4(fuel), tiles(oxidant), tiles4(oxidant), tiles(rate), velocity, sketch_x, sketch_y)


def solution(mesh):
    in_specs = (P("gy", "gz", None), P("gy", "gz", None), P("gy", "gz", None), P(), P(), P())
    out_specs = P("gy", None, "gz", None)
    return jax.shard_map(per_device, mesh=mesh, in_specs=in_specs, out_specs=out_specs, check_vma=False)
```

```python
import functools

import jax
import jax.numpy as jnp
from jax import lax
from jax.experimental import pallas as pl
from jax.experimental.pallas import tpu as pltpu
from jax.sharding import PartitionSpec as P

F32, BF16 = jnp.float32, jnp.bfloat16
MESH = pl.DeviceIdType.MESH
NX, NZL, NY = 4, 8, 4
DEVS = NX * NZL * NY
NT = 16
ROWS = 16


def roll(v, shift, axis):
    shift %= v.shape[axis]
    return pltpu.roll(v, shift, axis) if shift else v


def split(v):
    high = v.astype(BF16)
    return high, (v - high.astype(F32)).astype(BF16)


def dot(a, b, dims):
    return lax.dot_general(a, b, (dims, ((), ())), preferred_element_type=F32)


def kernel(
    fuel, fuel4, oxid, oxid4, rate, vel, sx, sy, out,
    F, RR, HB, VB, UF, RC, CC, CG, LT, SX, SXH, SXL, SY, SYT, SYH, SYL,
    P1, QM, ZD, PC, ZC, EA, ER, TA, TR, AE,
    s_vb, s_f, s_rr, s_sx, s_sy, far_s, far_r, ys, yr, ds, dr, zd_s, zd_r, zc_s, zc_r, ea_s, ea_r, ta_s, ta_r,
    zu, zd, go, near, ready,
):
    gy, gz = lax.axis_index("gy"), lax.axis_index("gz")
    x, zl, y = gy % NX, (gy // NX) % NZL, gy // (NX * NZL)
    core = gz % 2
    inner = (gz == 1) | (gz == 2)
    rim = jnp.logical_not(inner)
    partner = {"gy": gy, "gz": gz + 1 - 2 * core}
    opposite = {"gy": gy, "gz": 3 - gz}

    def at(yy, zz, xx):
        return {"gy": (yy * NZL + zz) * NX + xx, "gz": gz}

    def signal(sem, device):
        pl.semaphore_signal(sem, inc=1, device_id=device, device_id_type=MESH)

    def remote(src, dst, send, recv, device):
        return pltpu.make_async_remote_copy(
            src_ref=src, dst_ref=dst, send_sem=send, recv_sem=recv, device_id=device, device_id_type=MESH
        )

    def plane(p):
        return p + core * (3 - 2 * p)

    for f, src in enumerate((fuel4, oxid4)):
        for j in range(4):
            pltpu.make_async_copy(src.at[:, j, :, plane(0), :], VB.at[:, :, f * 4 + j, :], s_vb).start()
    barrier = pltpu.get_barrier_semaphore()
    above, below = at(y, zl + 1, x), at(y, zl - 1, x)
    rim_gz = 3 * (gz // 2)

    for a in range(NY):
        for b in range(NX):
            device = {"gy": (((y + a) % NY) * NZL + zl) * NX + (x + b) % NX, "gz": rim_gz}
            if a or b:
                signal(barrier, device)

    signal(barrier, partner)

    @pl.when((x == NX - 1) & (gy < DEVS - 1))
    def _():
        signal(barrier, {"gy": gy + 1, "gz": rim_gz})

    @pl.when((x == 0) & (gy > 0))
    def _():
        signal(barrier, {"gy": gy - 1, "gz": rim_gz})

    @pl.when(gz == 1)
    def _():
        signal(barrier, opposite)

    @pl.when(rim)
    def _():
        @pl.when(zl < NZL - 1)
        def _():
            signal(barrier, above)

        @pl.when(zl > 0)
        def _():
            signal(barrier, below)

        UF[...] = jnp.zeros_like(UF)
        ZC[...] = jnp.zeros_like(ZC)

    @pl.when(gy == 0)
    def _():
        F[0] = jnp.zeros((NT, 8, 128), F32)

    @pl.when(gy == DEVS - 1)
    def _():
        F[ROWS + 1] = jnp.zeros((NT, 8, 128), F32)

    pltpu.make_async_copy(VB, VB, s_vb).wait()
    for f, src in enumerate((fuel, oxid)):
        for p in (3, 0, 1, 2):
            pltpu.make_async_copy(src.at[:, :, plane(p), :], F.at[pl.ds(1, ROWS), :, f * 4 + p, :], s_f).start()
    for p in range(4):
        for f in range(2):
            pltpu.make_async_copy(rate.at[:, :, plane(p), :], RR.at[:, :, f * 4 + p, :], s_rr).start()
    pltpu.make_async_copy(sx, SX, s_sx).start()
    pltpu.make_async_copy(sy, SY, s_sy).start()

    @pl.when(gz == 1)
    def _():
        pl.semaphore_wait(barrier, 1)

    @pl.when(gz == 2)
    def _():
        pl.semaphore_wait(barrier, 2)
        signal(ready, opposite)

    ends = jnp.where((zl == 0) | (zl == NZL - 1), 32, 33)
    ends += jnp.where((x == 0) & (gy > 0), 2, 0) + jnp.where((x == NX - 1) & (gy < DEVS - 1), 2, 0)

    @pl.when(rim)
    def _():
        pl.semaphore_wait(barrier, ends)
        signal(near, partner)

        @pl.when(zl == 0)
        def _():
            signal(zu, above)

        @pl.when(zl == NZL - 1)
        def _():
            signal(zd, below)

    def far(g):
        return remote(VB.at[g], UF.at[g], far_s.at[g], far_r.at[g], opposite)

    @pl.when(gz == 2)
    def _():
        for g in range(4):
            far(g).start()

    def deck(f):
        return remote(
            F.at[pl.ds(1, ROWS), :, f * 4 + 3, :], HB.at[:, :, f * 4 + 3, :], ds.at[f], dr.at[f], partner
        )

    pltpu.make_async_copy(F.at[pl.ds(1, ROWS)], F.at[pl.ds(1, ROWS)], s_f).wait()
    for f in range(2):
        deck(f).start()

    north = {"gy": gy + 1, "gz": gz}
    south = {"gy": gy - 1, "gz": gz}

    def to_north():
        return remote(F.at[ROWS], F.at[0], ys.at[0], yr.at[0], north)

    def to_south():
        return remote(F.at[1], F.at[ROWS + 1], ys.at[1], yr.at[1], south)

    def send_rows():
        @pl.when(gy < DEVS - 1)
        def _():
            to_north().start()

        @pl.when(gy > 0)
        def _():
            to_south().start()

    @pl.when(gz == 1)
    def _():
        pl.semaphore_wait(near, 1)

    @pl.when(gz != 2)
    def _():
        send_rows()

    sub = lax.broadcasted_iota(jnp.int32, (8, 128), 0)
    lane = lax.broadcasted_iota(jnp.int32, (8, 128), 1)
    sp = sub % 4
    v0, v1 = 0.5 * vel[0], 0.5 * vel[1]
    v2 = 0.5 * vel[2] * (1 - 2 * core).astype(F32)
    alpha = jnp.where(sub < 4, 0.1, 0.05).astype(F32)
    zero = jnp.zeros((8, 128), F32)
    k0, kE, kW, kN, kS = 1.0 - 6.0 * alpha, alpha - v0, alpha + v0, alpha - v1, alpha + v1
    kP, kM = alpha - v2, alpha + v2
    sg = jnp.where(sub < 4, -1.0, 1.0).astype(F32)
    kMz = jnp.where(sp == 0, zero, kM)
    kPz = jnp.where(sp == 3, zero, kP)
    sgm = jnp.where(sp == 0, zero, sg)
    first, last = lane == 0, lane == 127

    def along_x(row):
        east = [roll(v, 127, 1) for v in row] + [zero]
        west = [zero] + [roll(v, 1, 1) for v in row]
        return [
            k0 * row[t]
            + kE * jnp.where(last, east[t + 1], east[t])
            + kW * jnp.where(first, west[t], west[t + 1])
            for t in range(NT)
        ]

    def compact(four):
        v = four[0]
        for j in range(1, 4):
            v = jnp.where(sp == j, roll(four[j], j, 0), v)
        return v

    pltpu.make_async_copy(sx, SX, s_sx).wait()

    @pl.loop(0, 8)
    def _(i):
        rows = pl.ds(pl.multiple_of(i * 16, 16), 16)
        SXH[rows, :], SXL[rows, :] = split(SX[rows, :])

    pltpu.make_async_copy(sy, SY, s_sy).wait()
    for b in range(16):
        SYT[b * 128 : (b + 1) * 128, :] = SY[:, b * 128 : (b + 1) * 128].T
    for r in range(ROWS):
        rows = slice(r * 128, (r + 1) * 128)
        SYH[rows, :], SYL[rows, :] = split(SYT[pl.ds(r, 128, stride=16), :])

    def project(read, rows):
        total = jnp.zeros((rows, 128), F32)
        for c in range(NT // 2):
            high, low = split(jnp.concatenate([read(2 * c), read(2 * c + 1)], axis=1))
            cols = slice(c * 256, (c + 1) * 256)
            nt = ((1,), (1,))
            both = dot(jnp.concatenate([high, low], axis=0), SXH[:, cols], nt)
            total += both[:rows] + both[rows:] + dot(high, SXL[:, cols], nt)
        return total

    pltpu.make_async_copy(RR, RR, s_rr).wait()
    for f in range(2):
        deck(f).wait_recv()

    @pl.loop(0, ROWS)
    def _(r):
        kn, ks = jnp.where(r == ROWS - 1, zero, kN), jnp.where(r == 0, zero, kS)
        rn, rs = jnp.minimum(r + 2, ROWS), jnp.maximum(r, 1)
        row = [F[r + 1, t] for t in range(NT)]
        ahead = along_x(row)
        after = []
        for t in range(NT):
            v = row[t]
            up = jnp.where(sp == 3, HB[r, t], roll(v, 7, 0))
            c = ahead[t] + kn * F[rn, t] + ks * F[rs, t] + kP * up + kMz * roll(v, 1, 0)
            c += sg * RR[r, t] * v * roll(v, 4, 0)
            CG[0, r, t] = c
            after.append(c)
        for t, g in enumerate(along_x(after)):
            c = after[t]
            CG[1, r, t] = g + sgm * RR[r, t] * c * roll(c, 4, 0)

    def to_partner():
        return remote(P1, ZD, zd_s, zd_r, partner)

    def to_opposite():
        return remote(PC, ZC, zc_s, zc_r, opposite)

    def compact_rows(g):
        for t in range(NT):
            CC[g, t] = compact([CG[0, 4 * g + j, t] for j in range(4)])

    @pl.loop(0, 4)
    def _(g):
        compact_rows(g)
        for t in range(NT):
            RC[g, t] = compact([RR[4 * g + j, t] for j in range(4)])

    local = project(lambda t: jnp.concatenate([VB[:, t].reshape(32, 128), CC[:, t].reshape(32, 128)], axis=0), 64)
    P0 = local[:32].reshape(4, 8, 128)
    PC[...] = local[32:].reshape(4, 8, 128)

    @pl.when(gz == 1)
    def _():
        pl.semaphore_wait(ready, 1)
        to_opposite().start()
        for g in range(4):
            far(g).start()

    @pl.when(gz == 2)
    def _():
        to_opposite().start()

    @pl.when(gz == 2)
    def _():
        pl.semaphore_wait(near, 1)
        send_rows()

    middle = (ROWS - 2) * 8
    early = project(lambda t: CG[:, 1 : ROWS - 1, t].reshape(2 * middle, 128), 2 * middle)
    P1[1 : ROWS - 1] = early[:middle].reshape(ROWS - 2, 8, 128)
    QM[...] = early[middle:].reshape(ROWS - 2, 8, 128)

    @pl.when(rim)
    def _():
        @pl.when((zl > 0) & (zl < NZL // 2))
        def _():
            pl.semaphore_wait(zu, 1)
            signal(zu, above)
            pl.semaphore_wait(zd, 1)
            signal(zd, below)

        @pl.when((zl < NZL - 1) & (zl >= NZL // 2))
        def _():
            pl.semaphore_wait(zd, 1)
            signal(zd, below)
            pl.semaphore_wait(zu, 1)
            signal(zu, above)

        @pl.when(zl == 0)
        def _():
            pl.semaphore_wait(zd, 1)

        @pl.when(zl == NZL - 1)
        def _():
            pl.semaphore_wait(zu, 1)

        signal(go, partner)

    @pl.when(gy > 0)
    def _():
        to_north().wait_recv()

    @pl.when(gy < DEVS - 1)
    def _():
        to_south().wait_recv()

    for r, halo, k in ((0, 0, kS), (ROWS - 1, ROWS + 1, kN)):
        after = [CG[0, r, t] + k * F[halo, t] for t in range(NT)]
        for t, g in enumerate(along_x(after)):
            c = after[t]
            CG[0, r, t] = c
            CG[1, r, t] = g + sgm * RR[r, t] * c * roll(c, 4, 0)
    compact_rows(0)
    compact_rows(3)

    brims = project(
        lambda t: jnp.concatenate([CG[0, 0, t], CG[0, ROWS - 1, t], CG[1, 0, t], CG[1, ROWS - 1, t]], axis=0), 32
    )
    P1[0] = brims[:8]
    P1[ROWS - 1] = brims[8:16]
    to_partner().start()
    Q = [brims[16:24]] + [QM[r] for r in range(ROWS - 2)] + [brims[24:]]

    to_partner().wait_recv()
    rows = []
    for r in range(ROWS):
        v = P1[r]
        e = Q[r] + kPz * roll(v, 7, 0) + kMz * roll(v, 1, 0) + jnp.where(sp == 3, kP * ZD[r], zero)
        if r < ROWS - 1:
            e += kN * P1[r + 1]
        if r > 0:
            e += kS * P1[r - 1]
        rows.append(e)
    EA[...] = jnp.concatenate(rows, axis=0).T

    def exchange(src, dst, send, recv):
        def one(to):
            remote(src.at[pl.ds(to, 1), :], dst.at[pl.ds(gy, 1), :], send, recv, {"gy": to, "gz": gz}).start()

        @pl.loop(0, NZL)
        def _(n):
            zz = jnp.where(zl < NZL // 2, NZL - 1 - n, n)
            for m in range(1, NX * NY):
                one((((y + m // NX) % NY) * NZL + zz) * NX + (x + m % NX) % NX)

            @pl.when(zz != zl)
            def _():
                one((y * NZL + zz) * NX + x)

        dst[pl.ds(gy, 1), :] = src[pl.ds(gy, 1), :]

    def all_rows(src, dst, send, recv):
        return remote(src.at[pl.ds(0, DEVS - 1), :], dst.at[pl.ds(0, DEVS - 1), :], send, recv, partner)

    @pl.when(inner)
    def _():
        pl.semaphore_wait(go, 1)

    exchange(EA, ER, ea_s, ea_r)

    for g in range(4):
        @pl.when(inner)
        def _():
            far(g).wait_recv()

        delta = [kM * UF[g, t] for t in range(NT)]
        for t, q in enumerate(along_x(delta)):
            c = CC[g, t] + delta[t]
            LT[g, t] = delta[t]
            LT[4 + g, t] = q + sg * RC[g, t] * c * roll(c, 4, 0)
    late = project(lambda t: LT[:, t].reshape(64, 128), 64).reshape(8, 8, 128)

    @pl.when(inner)
    def _():
        to_opposite().wait_recv()

    kF = kM * kP * jnp.where(inner, 1.0, 0.0).astype(F32)
    D = [late[g] for g in range(4)]
    X = []
    for g in range(4):
        v = late[4 + g] + kF * P0[g] + kM * ZC[g]
        ahead = roll(D[g + 1], 3, 0) if g < 3 else zero
        behind = roll(D[g - 1], 5, 0) if g > 0 else zero
        v += kN * jnp.where(sp == 3, ahead, roll(D[g], 7, 0))
        v += kS * jnp.where(sp == 0, behind, roll(D[g], 1, 0))
        X.append(v)
    low_edge = kN * P1[0] + jnp.where(sp == 0, 2.0 * kN * D[0], zero)
    high_edge = kS * P1[ROWS - 1] + jnp.where(sp == 0, 2.0 * kS * roll(D[3], 5, 0), zero)
    spare = [low_edge, roll(low_edge, 2, 0), high_edge, roll(high_edge, 2, 0)] + [zero] * (ROWS - 4)
    rows = []
    for r in range(ROWS):
        g, j = divmod(r, 4)
        v = jnp.where(sp == 0, roll(X[g], 8 - j, 0), spare[r])
        rows.append(jnp.where(sp == 1, kM * roll(D[g], 9 - j, 0), v))
    TA[...] = jnp.concatenate(rows, axis=0).T
    exchange(TA, TR, ta_s, ta_r)

    all_rows(EA, ER, ea_s, ea_r).wait_recv()
    AE[...] = ER[...].T
    all_rows(TA, TR, ta_s, ta_r).wait_recv()
    T = TR[...].T
    tail = [T[8 * r : 8 * r + 8] for r in range(ROWS)]
    low_edge = jnp.where(sp >= 2, tail[0], roll(tail[1], 6, 0))
    high_edge = jnp.where(sp >= 2, tail[2], roll(tail[3], 6, 0))
    A = [AE[8 * r : 8 * r + 8, :] + jnp.where(sp < 2, tail[r], zero) for r in range(ROWS)]
    A[ROWS - 1] += jnp.where(last, zero, roll(low_edge, 127, 1))
    A[0] += jnp.where(first, zero, roll(high_edge, 1, 1))
    high, low = split(jnp.concatenate(A, axis=1))
    nn = ((1,), (0,))
    both = dot(jnp.concatenate([high, low], axis=0), SYH[...], nn)
    res = both[:8] + both[8:] + dot(high, SYL[...], nn)
    flipped = jnp.where(
        sp == 0, roll(res, 5, 0), jnp.where(sp == 1, roll(res, 7, 0), jnp.where(sp == 2, roll(res, 1, 0), roll(res, 3, 0)))
    )
    res = jnp.where(jnp.full((8, 128), core) == 1, flipped, res)
    out[0, 0] = res[:4]
    out[0, 1] = res[4:]

    @pl.when(inner)
    def _():
        for g in range(4):
            far(g).wait_send()
        to_opposite().wait_send()

    for f in range(2):
        deck(f).wait_send()

    @pl.when(gy < DEVS - 1)
    def _():
        to_north().wait_send()

    @pl.when(gy > 0)
    def _():
        to_south().wait_send()

    to_partner().wait_send()
    all_rows(EA, ER, ea_s, ea_r).wait_send()
    all_rows(TA, TR, ta_s, ta_r).wait_send()


def per_device(fuel, oxidant, rate, velocity, sketch_x, sketch_y):
    def tiles(a):
        return a.reshape(ROWS, 4, NT, 128).transpose(0, 2, 1, 3)

    def tiles4(a):
        return tiles(a).reshape(4, 4, NT, 4, 128)

    vm = lambda *shape, kind=F32: pltpu.VMEM(shape, kind)
    dma, one = pltpu.SemaphoreType.DMA, pltpu.SemaphoreType.REGULAR
    whole = (ROWS, NT, 8, 128)
    plane = (4, NT, 8, 128)
    return pl.pallas_call(
        kernel,
        out_shape=jax.ShapeDtypeStruct((1, 2, 4, 128), F32),
        in_specs=[pl.BlockSpec(memory_space=pl.ANY)] * 5
        + [pl.BlockSpec(memory_space=pltpu.SMEM)]
        + [pl.BlockSpec(memory_space=pl.ANY)] * 2,
        out_specs=pl.BlockSpec(memory_space=pltpu.VMEM),
        scratch_shapes=[
            vm(ROWS + 2, NT, 8, 128), vm(*whole), vm(*whole), vm(*plane), vm(*plane), vm(*plane), vm(*plane),
            vm(2, *whole), vm(8, NT, 8, 128), vm(128, 2048), vm(128, 2048, kind=BF16), vm(128, 2048, kind=BF16),
            vm(128, 2048), vm(2048, 128), vm(2048, 128, kind=BF16), vm(2048, 128, kind=BF16),
            vm(ROWS, 8, 128), vm(ROWS - 2, 8, 128), vm(ROWS, 8, 128), vm(4, 8, 128), vm(4, 8, 128),
            vm(128, 128), vm(128, 128), vm(128, 128), vm(128, 128), vm(128, 128),
            dma, dma, dma, dma, dma, dma((4,)), dma((4,)), dma((2,)), dma((2,)), dma((2,)), dma((2,)),
            dma, dma, dma, dma, dma, dma, dma, dma,
            one, one, one, one, one,
        ],
        compiler_params=pltpu.CompilerParams(collective_id=0, has_side_effects=True),
        name="advect_sketch",
    )(tiles(fuel), tiles4(fuel), tiles(oxidant), tiles4(oxidant), tiles(rate), velocity, sketch_x, sketch_y)


def solution(mesh):
    in_specs = (P("gy", "gz", None), P("gy", "gz", None), P("gy", "gz", None), P(), P(), P())
    out_specs = P("gy", None, "gz", None)
    return jax.shard_map(per_device, mesh=mesh, in_specs=in_specs, out_specs=out_specs, check_vma=False)
```

```python
import functools

import jax
import jax.numpy as jnp
from jax import lax
from jax.experimental import pallas as pl
from jax.experimental.pallas import tpu as pltpu
from jax.sharding import PartitionSpec as P

F32, BF16 = jnp.float32, jnp.bfloat16
MESH = pl.DeviceIdType.MESH
NX, NZL, NY = 4, 8, 4
DEVS = NX * NZL * NY
NT = 16
ROWS = 16


def roll(v, shift, axis):
    shift %= v.shape[axis]
    return pltpu.roll(v, shift, axis) if shift else v


def split(v):
    high = v.astype(BF16)
    return high, (v - high.astype(F32)).astype(BF16)


def dot(a, b, dims):
    return lax.dot_general(a, b, (dims, ((), ())), preferred_element_type=F32)


def kernel(
    fuel, fuel4, oxid, oxid4, rate, vel, sx, sy, out,
    F, RR, HB, VB, UF, RC, CC, CG, LT, SX, SXH, SXL, SY, SYT, SYH, SYL,
    P1, QM, ZD, PC, ZC, EA, ER, TA, TR, AE,
    s_vb, s_f, s_rr, s_sx, s_sy, far_s, far_r, ys, yr, ds, dr, zd_s, zd_r, zc_s, zc_r, ea_s, ea_r, ta_s, ta_r,
    zu, zd, go, near, ready,
):
    gy, gz = lax.axis_index("gy"), lax.axis_index("gz")
    x, zl, y = gy % NX, (gy // NX) % NZL, gy // (NX * NZL)
    core = gz % 2
    inner = (gz == 1) | (gz == 2)
    rim = jnp.logical_not(inner)
    partner = {"gy": gy, "gz": gz + 1 - 2 * core}
    opposite = {"gy": gy, "gz": 3 - gz}

    def at(yy, zz, xx):
        return {"gy": (yy * NZL + zz) * NX + xx, "gz": gz}

    def signal(sem, device):
        pl.semaphore_signal(sem, inc=1, device_id=device, device_id_type=MESH)

    def remote(src, dst, send, recv, device):
        return pltpu.make_async_remote_copy(
            src_ref=src, dst_ref=dst, send_sem=send, recv_sem=recv, device_id=device, device_id_type=MESH
        )

    def plane(p):
        return p + core * (3 - 2 * p)

    for f, src in enumerate((fuel4, oxid4)):
        for j in range(4):
            pltpu.make_async_copy(src.at[:, j, :, plane(0), :], VB.at[:, :, f * 4 + j, :], s_vb).start()
    barrier = pltpu.get_barrier_semaphore()
    above, below = at(y, zl + 1, x), at(y, zl - 1, x)
    rim_gz = 3 * (gz // 2)

    for a in range(NY):
        for b in range(NX):
            device = {"gy": (((y + a) % NY) * NZL + zl) * NX + (x + b) % NX, "gz": rim_gz}
            if a or b:
                signal(barrier, device)

    signal(barrier, partner)

    @pl.when((x == NX - 1) & (gy < DEVS - 1))
    def _():
        signal(barrier, {"gy": gy + 1, "gz": rim_gz})

    @pl.when((x == 0) & (gy > 0))
    def _():
        signal(barrier, {"gy": gy - 1, "gz": rim_gz})

    @pl.when(gz == 1)
    def _():
        signal(barrier, opposite)

    @pl.when(rim)
    def _():
        @pl.when(zl < NZL - 1)
        def _():
            signal(barrier, above)

        @pl.when(zl > 0)
        def _():
            signal(barrier, below)

        UF[...] = jnp.zeros_like(UF)
        ZC[...] = jnp.zeros_like(ZC)

    @pl.when(gy == 0)
    def _():
        F[0] = jnp.zeros((NT, 8, 128), F32)

    @pl.when(gy == DEVS - 1)
    def _():
        F[ROWS + 1] = jnp.zeros((NT, 8, 128), F32)

    pltpu.make_async_copy(VB, VB, s_vb).wait()
    for f, src in enumerate((fuel, oxid)):
        for p in (3, 0, 1, 2):
            pltpu.make_async_copy(src.at[:, :, plane(p), :], F.at[pl.ds(1, ROWS), :, f * 4 + p, :], s_f).start()
    for p in range(4):
        for f in range(2):
            pltpu.make_async_copy(rate.at[:, :, plane(p), :], RR.at[:, :, f * 4 + p, :], s_rr).start()
    pltpu.make_async_copy(sx, SX, s_sx).start()
    pltpu.make_async_copy(sy, SY, s_sy).start()

    @pl.when(gz == 1)
    def _():
        pl.semaphore_wait(barrier, 1)

    @pl.when(gz == 2)
    def _():
        pl.semaphore_wait(barrier, 2)
        signal(ready, opposite)

    ends = jnp.where((zl == 0) | (zl == NZL - 1), 32, 33)
    ends += jnp.where((x == 0) & (gy > 0), 2, 0) + jnp.where((x == NX - 1) & (gy < DEVS - 1), 2, 0)

    @pl.when(rim)
    def _():
        pl.semaphore_wait(barrier, ends)
        signal(near, partner)

        @pl.when(zl == 0)
        def _():
            signal(zu, above)

        @pl.when(zl == NZL - 1)
        def _():
            signal(zd, below)

    def far(g):
        return remote(VB.at[g], UF.at[g], far_s.at[g], far_r.at[g], opposite)

    @pl.when(gz == 2)
    def _():
        for g in range(4):
            far(g).start()

    def deck(f):
        return remote(
            F.at[pl.ds(1, ROWS), :, f * 4 + 3, :], HB.at[:, :, f * 4 + 3, :], ds.at[f], dr.at[f], partner
        )

    pltpu.make_async_copy(F.at[pl.ds(1, ROWS)], F.at[pl.ds(1, ROWS)], s_f).wait()
    for f in range(2):
        deck(f).start()

    north = {"gy": gy + 1, "gz": gz}
    south = {"gy": gy - 1, "gz": gz}

    def to_north():
        return remote(F.at[ROWS], F.at[0], ys.at[0], yr.at[0], north)

    def to_south():
        return remote(F.at[1], F.at[ROWS + 1], ys.at[1], yr.at[1], south)

    def send_rows():
        @pl.when(gy < DEVS - 1)
        def _():
            to_north().start()

        @pl.when(gy > 0)
        def _():
            to_south().start()

    @pl.when(gz == 1)
    def _():
        pl.semaphore_wait(near, 1)

    @pl.when(gz != 2)
    def _():
        send_rows()

    sub = lax.broadcasted_iota(jnp.int32, (8, 128), 0)
    lane = lax.broadcasted_iota(jnp.int32, (8, 128), 1)
    sp = sub % 4
    v0, v1 = 0.5 * vel[0], 0.5 * vel[1]
    v2 = 0.5 * vel[2] * (1 - 2 * core).astype(F32)
    alpha = jnp.where(sub < 4, 0.1, 0.05).astype(F32)
    zero = jnp.zeros((8, 128), F32)
    k0, kE, kW, kN, kS = 1.0 - 6.0 * alpha, alpha - v0, alpha + v0, alpha - v1, alpha + v1
    kP, kM = alpha - v2, alpha + v2
    sg = jnp.where(sub < 4, -1.0, 1.0).astype(F32)
    kMz = jnp.where(sp == 0, zero, kM)
    kPz = jnp.where(sp == 3, zero, kP)
    sgm = jnp.where(sp == 0, zero, sg)
    first, last = lane == 0, lane == 127

    def along_x(row):
        east = [roll(v, 127, 1) for v in row] + [zero]
        west = [zero] + [roll(v, 1, 1) for v in row]
        return [
            k0 * row[t]
            + kE * jnp.where(last, east[t + 1], east[t])
            + kW * jnp.where(first, west[t], west[t + 1])
            for t in range(NT)
        ]

    def compact(four):
        v = four[0]
        for j in range(1, 4):
            v = jnp.where(sp == j, roll(four[j], j, 0), v)
        return v

    pltpu.make_async_copy(sx, SX, s_sx).wait()

    @pl.loop(0, 8)
    def _(i):
        rows = pl.ds(pl.multiple_of(i * 16, 16), 16)
        SXH[rows, :], SXL[rows, :] = split(SX[rows, :])

    pltpu.make_async_copy(sy, SY, s_sy).wait()
    for b in range(16):
        SYT[b * 128 : (b + 1) * 128, :] = SY[:, b * 128 : (b + 1) * 128].T
    for r in range(ROWS):
        rows = slice(r * 128, (r + 1) * 128)
        SYH[rows, :], SYL[rows, :] = split(SYT[pl.ds(r, 128, stride=16), :])

    def project(read, rows):
        total = jnp.zeros((rows, 128), F32)
        for c in range(NT // 2):
            high, low = split(jnp.concatenate([read(2 * c), read(2 * c + 1)], axis=1))
            cols = slice(c * 256, (c + 1) * 256)
            nt = ((1,), (1,))
            both = dot(jnp.concatenate([high, low], axis=0), SXH[:, cols], nt)
            total += both[:rows] + both[rows:] + dot(high, SXL[:, cols], nt)
        return total

    pltpu.make_async_copy(RR, RR, s_rr).wait()
    for f in range(2):
        deck(f).wait_recv()

    @pl.loop(0, ROWS)
    def _(r):
        kn, ks = jnp.where(r == ROWS - 1, zero, kN), jnp.where(r == 0, zero, kS)
        rn, rs = jnp.minimum(r + 2, ROWS), jnp.maximum(r, 1)
        row = [F[r + 1, t] for t in range(NT)]
        ahead = along_x(row)
        after = []
        for t in range(NT):
            v = row[t]
            up = jnp.where(sp == 3, HB[r, t], roll(v, 7, 0))
            c = ahead[t] + kn * F[rn, t] + ks * F[rs, t] + kP * up + kMz * roll(v, 1, 0)
            c += sg * RR[r, t] * v * roll(v, 4, 0)
            CG[0, r, t] = c
            after.append(c)
        for t, g in enumerate(along_x(after)):
            c = after[t]
            CG[1, r, t] = g + sgm * RR[r, t] * c * roll(c, 4, 0)

    def to_partner():
        return remote(P1, ZD, zd_s, zd_r, partner)

    def to_opposite():
        return remote(PC, ZC, zc_s, zc_r, opposite)

    def compact_rows(g):
        for t in range(NT):
            CC[g, t] = compact([CG[0, 4 * g + j, t] for j in range(4)])

    @pl.loop(0, 4)
    def _(g):
        compact_rows(g)
        for t in range(NT):
            RC[g, t] = compact([RR[4 * g + j, t] for j in range(4)])

    local = project(lambda t: jnp.concatenate([VB[:, t].reshape(32, 128), CC[:, t].reshape(32, 128)], axis=0), 64)
    P0 = local[:32].reshape(4, 8, 128)
    PC[...] = local[32:].reshape(4, 8, 128)

    @pl.when(gz == 1)
    def _():
        pl.semaphore_wait(ready, 1)
        to_opposite().start()
        for g in range(4):
            far(g).start()

    @pl.when(gz == 2)
    def _():
        to_opposite().start()

    @pl.when(gz == 2)
    def _():
        pl.semaphore_wait(near, 1)
        send_rows()

    middle = (ROWS - 2) * 8
    early = project(lambda t: CG[:, 1 : ROWS - 1, t].reshape(2 * middle, 128), 2 * middle)
    P1[1 : ROWS - 1] = early[:middle].reshape(ROWS - 2, 8, 128)
    QM[...] = early[middle:].reshape(ROWS - 2, 8, 128)

    @pl.when(rim)
    def _():
        @pl.when((zl > 0) & (zl < NZL // 2))
        def _():
            pl.semaphore_wait(zu, 1)
            signal(zu, above)
            pl.semaphore_wait(zd, 1)
            signal(zd, below)

        @pl.when((zl < NZL - 1) & (zl >= NZL // 2))
        def _():
            pl.semaphore_wait(zd, 1)
            signal(zd, below)
            pl.semaphore_wait(zu, 1)
            signal(zu, above)

        @pl.when(zl == 0)
        def _():
            pl.semaphore_wait(zd, 1)

        @pl.when(zl == NZL - 1)
        def _():
            pl.semaphore_wait(zu, 1)

        signal(go, partner)

    @pl.when(gy > 0)
    def _():
        to_north().wait_recv()

    @pl.when(gy < DEVS - 1)
    def _():
        to_south().wait_recv()

    for r, halo, k in ((0, 0, kS), (ROWS - 1, ROWS + 1, kN)):
        after = [CG[0, r, t] + k * F[halo, t] for t in range(NT)]
        for t, g in enumerate(along_x(after)):
            c = after[t]
            CG[0, r, t] = c
            CG[1, r, t] = g + sgm * RR[r, t] * c * roll(c, 4, 0)
    compact_rows(0)
    compact_rows(3)

    brims = project(
        lambda t: jnp.concatenate([CG[0, 0, t], CG[0, ROWS - 1, t], CG[1, 0, t], CG[1, ROWS - 1, t]], axis=0), 32
    )
    P1[0] = brims[:8]
    P1[ROWS - 1] = brims[8:16]
    to_partner().start()
    Q = [brims[16:24]] + [QM[r] for r in range(ROWS - 2)] + [brims[24:]]

    to_partner().wait_recv()
    rows = []
    for r in range(ROWS):
        v = P1[r]
        e = Q[r] + kPz * roll(v, 7, 0) + kMz * roll(v, 1, 0) + jnp.where(sp == 3, kP * ZD[r], zero)
        if r < ROWS - 1:
            e += kN * P1[r + 1]
        if r > 0:
            e += kS * P1[r - 1]
        rows.append(e)
    EA[...] = jnp.concatenate(rows, axis=0).T

    def exchange(src, dst, send, recv):
        def one(to):
            remote(src.at[pl.ds(to, 1), :], dst.at[pl.ds(gy, 1), :], send, recv, {"gy": to, "gz": gz}).start()

        @pl.loop(0, NZL)
        def _(n):
            zz = jnp.where(zl < NZL // 2, NZL - 1 - n, n)
            for m in range(NX * NY):
                to = ((m // NX) * NZL + zz) * NX + m % NX

                @pl.when(to != gy)
                def _():
                    one(to)

        dst[pl.ds(gy, 1), :] = src[pl.ds(gy, 1), :]

    def all_rows(src, dst, send, recv):
        return remote(src.at[pl.ds(0, DEVS - 1), :], dst.at[pl.ds(0, DEVS - 1), :], send, recv, partner)

    @pl.when(inner)
    def _():
        pl.semaphore_wait(go, 1)

    exchange(EA, ER, ea_s, ea_r)

    for g in range(4):
        @pl.when(inner)
        def _():
            far(g).wait_recv()

        delta = [kM * UF[g, t] for t in range(NT)]
        for t, q in enumerate(along_x(delta)):
            c = CC[g, t] + delta[t]
            LT[g, t] = delta[t]
            LT[4 + g, t] = q + sg * RC[g, t] * c * roll(c, 4, 0)
    late = project(lambda t: LT[:, t].reshape(64, 128), 64).reshape(8, 8, 128)

    @pl.when(inner)
    def _():
        to_opposite().wait_recv()

    kF = kM * kP * jnp.where(inner, 1.0, 0.0).astype(F32)
    D = [late[g] for g in range(4)]
    X = []
    for g in range(4):
        v = late[4 + g] + kF * P0[g] + kM * ZC[g]
        ahead = roll(D[g + 1], 3, 0) if g < 3 else zero
        behind = roll(D[g - 1], 5, 0) if g > 0 else zero
        v += kN * jnp.where(sp == 3, ahead, roll(D[g], 7, 0))
        v += kS * jnp.where(sp == 0, behind, roll(D[g], 1, 0))
        X.append(v)
    low_edge = kN * P1[0] + jnp.where(sp == 0, 2.0 * kN * D[0], zero)
    high_edge = kS * P1[ROWS - 1] + jnp.where(sp == 0, 2.0 * kS * roll(D[3], 5, 0), zero)
    spare = [low_edge, roll(low_edge, 2, 0), high_edge, roll(high_edge, 2, 0)] + [zero] * (ROWS - 4)
    rows = []
    for r in range(ROWS):
        g, j = divmod(r, 4)
        v = jnp.where(sp == 0, roll(X[g], 8 - j, 0), spare[r])
        rows.append(jnp.where(sp == 1, kM * roll(D[g], 9 - j, 0), v))
    TA[...] = jnp.concatenate(rows, axis=0).T
    exchange(TA, TR, ta_s, ta_r)

    all_rows(EA, ER, ea_s, ea_r).wait_recv()
    AE[...] = ER[...].T
    all_rows(TA, TR, ta_s, ta_r).wait_recv()
    T = TR[...].T
    tail = [T[8 * r : 8 * r + 8] for r in range(ROWS)]
    low_edge = jnp.where(sp >= 2, tail[0], roll(tail[1], 6, 0))
    high_edge = jnp.where(sp >= 2, tail[2], roll(tail[3], 6, 0))
    A = [AE[8 * r : 8 * r + 8, :] + jnp.where(sp < 2, tail[r], zero) for r in range(ROWS)]
    A[ROWS - 1] += jnp.where(last, zero, roll(low_edge, 127, 1))
    A[0] += jnp.where(first, zero, roll(high_edge, 1, 1))
    high, low = split(jnp.concatenate(A, axis=1))
    nn = ((1,), (0,))
    both = dot(jnp.concatenate([high, low], axis=0), SYH[...], nn)
    res = both[:8] + both[8:] + dot(high, SYL[...], nn)
    flipped = jnp.where(
        sp == 0, roll(res, 5, 0), jnp.where(sp == 1, roll(res, 7, 0), jnp.where(sp == 2, roll(res, 1, 0), roll(res, 3, 0)))
    )
    res = jnp.where(jnp.full((8, 128), core) == 1, flipped, res)
    out[0, 0] = res[:4]
    out[0, 1] = res[4:]

    @pl.when(inner)
    def _():
        for g in range(4):
            far(g).wait_send()
        to_opposite().wait_send()

    for f in range(2):
        deck(f).wait_send()

    @pl.when(gy < DEVS - 1)
    def _():
        to_north().wait_send()

    @pl.when(gy > 0)
    def _():
        to_south().wait_send()

    to_partner().wait_send()
    all_rows(EA, ER, ea_s, ea_r).wait_send()
    all_rows(TA, TR, ta_s, ta_r).wait_send()


def per_device(fuel, oxidant, rate, velocity, sketch_x, sketch_y):
    def tiles(a):
        return a.reshape(ROWS, 4, NT, 128).transpose(0, 2, 1, 3)

    def tiles4(a):
        return tiles(a).reshape(4, 4, NT, 4, 128)

    vm = lambda *shape, kind=F32: pltpu.VMEM(shape, kind)
    dma, one = pltpu.SemaphoreType.DMA, pltpu.SemaphoreType.REGULAR
    whole = (ROWS, NT, 8, 128)
    plane = (4, NT, 8, 128)
    return pl.pallas_call(
        kernel,
        out_shape=jax.ShapeDtypeStruct((1, 2, 4, 128), F32),
        in_specs=[pl.BlockSpec(memory_space=pl.ANY)] * 5
        + [pl.BlockSpec(memory_space=pltpu.SMEM)]
        + [pl.BlockSpec(memory_space=pl.ANY)] * 2,
        out_specs=pl.BlockSpec(memory_space=pltpu.VMEM),
        scratch_shapes=[
            vm(ROWS + 2, NT, 8, 128), vm(*whole), vm(*whole), vm(*plane), vm(*plane), vm(*plane), vm(*plane),
            vm(2, *whole), vm(8, NT, 8, 128), vm(128, 2048), vm(128, 2048, kind=BF16), vm(128, 2048, kind=BF16),
            vm(128, 2048), vm(2048, 128), vm(2048, 128, kind=BF16), vm(2048, 128, kind=BF16),
            vm(ROWS, 8, 128), vm(ROWS - 2, 8, 128), vm(ROWS, 8, 128), vm(4, 8, 128), vm(4, 8, 128),
            vm(128, 128), vm(128, 128), vm(128, 128), vm(128, 128), vm(128, 128),
            dma, dma, dma, dma, dma, dma((4,)), dma((4,)), dma((2,)), dma((2,)), dma((2,)), dma((2,)),
            dma, dma, dma, dma, dma, dma, dma, dma,
            one, one, one, one, one,
        ],
        compiler_params=pltpu.CompilerParams(collective_id=0, has_side_effects=True),
        name="advect_sketch",
    )(tiles(fuel), tiles4(fuel), tiles(oxidant), tiles4(oxidant), tiles(rate), velocity, sketch_x, sketch_y)


def solution(mesh):
    in_specs = (P("gy", "gz", None), P("gy", "gz", None), P("gy", "gz", None), P(), P(), P())
    out_specs = P("gy", None, "gz", None)
    return jax.shard_map(per_device, mesh=mesh, in_specs=in_specs, out_specs=out_specs, check_vma=False)
```
